32 devices in a mesh: ctx: 16 (over z, y, core), head: 2 (over x).
Axes of the slice: x: 2, y: 2, z: 4, core: 2. Of those that a mesh axis runs over, the one named last changes fastest.
Arguments:
- queries: bfloat16 [2048, 2048], P('ctx', 'head'), may hold values from -100 to 100
- keys: bfloat16 [2048, 2048], P('ctx', 'head'), may hold values from -50 to 50
- values: bfloat16 [2048, 2048], P('ctx', 'head'), may hold values from -6 to 6
- out_weight: bfloat16 [2048, 4096], P('head'), may hold values from -0.125 to 0.125
- mixed_grad: bfloat16 [2048, 4096], P('ctx', 'head'), may hold values from -6 to 6
- lengths: int32 [16], replicated, may hold values from 1 to 384, 2048 in all
- dilation: int32 [16], P('head'), may hold values from 1 to 8
Outputs:
- mixed: bfloat16 [2048, 4096], P('ctx', 'head')
- grad_queries: bfloat16 [2048, 2048], P('ctx', 'head')
- grad_keys: bfloat16 [2048, 2048], P('ctx', 'head')
- grad_values: bfloat16 [2048, 2048], P('ctx', 'head')
The draws below stay inside these ranges and needn't reach their ends.
Inputs may be any that keep to these rules, and one draw needn't show every extreme that they name: The lengths sum to 2048, and the longest document has exactly 384 tokens.
All inputs are finite; a program needn't handle non-finite values.
Results may differ from the reference program's by a relative error of at most 0.029.
Values may be sent and summed in bfloat16 or wider, within the bound.
A program may use at most 64 MiB of HBM per device.

```python
import math
import jax
import jax.numpy as jnp
import numpy as np
from jax import lax

D = 4096
HEADS = 16
HD = 128
HALF = 32
MAXD = 8
TOK_DEV = 128
TOKENS = 2048
DOCS = 16


def draw_queries(key, part):
    drawn = jax.random.normal(jax.random.fold_in(key, 11), (TOKENS, HEADS * HD), jnp.float32)
    return drawn.astype(jnp.bfloat16)


def draw_keys(key, part):
    drawn = jax.random.normal(jax.random.fold_in(key, 23), (TOKENS, HEADS * HD), jnp.float32)
    return drawn.astype(jnp.bfloat16)


def plant(entries, stream_key, smallest, high):
    shape = entries.shape
    spot = [jax.random.randint(jax.random.fold_in(stream_key, axis), (), 0, shape[axis]) for axis in range(len(shape))]
    entries = entries.at[tuple(spot)].set(smallest)
    longest = shape.index(max(shape))
    spot[longest] = (spot[longest] + 1) % shape[longest]
    return entries.at[tuple(spot)].set(high)


def block_scale(own_key, dims, shards, smallest, high):
    def one(axis_at, blocks):
        draws = jax.random.uniform(jax.random.fold_in(jax.random.fold_in(own_key, 6), axis_at), (blocks,), jnp.float32, smallest / len(shards), high / len(shards))
        return jnp.repeat(jnp.exp(draws), dims[axis_at] // blocks).reshape((-1,) + (1,) * (len(dims) - axis_at - 1))

    factor_of = one(*shards[0])
    for cut in shards[1:]:
        factor_of = factor_of * one(*cut)
    return factor_of


def split_up(amount, total, most, slope):
    portions = [(1 << 20) // math.isqrt(rank ** slope) + 1 for rank in range(2, amount + 1)]
    spare, given = total - most - (amount - 1), [1] * (amount - 1)
    while spare > 0:
        free = [i for i in range(amount - 1) if given[i] < most]
        pool, budget = sum([portions[i] for i in free]), spare
        for i in free:
            extra = min(most - given[i], max(1, budget * portions[i] // pool), spare)
            given[i] = given[i] + extra
            spare = spare - extra
    return np.array([most] + given)


def ragged(stream_key, amount, total, most, skew):
    if amount == 2:
        one = jax.random.randint(stream_key, (), max(1, total - most), min(most, total - 1) + 1)
        return jnp.stack([one, total - one])
    sizes = jnp.asarray(split_up(amount, total, most, skew), jnp.int32)
    twos = (amount - 1) // 2
    source_of, taker = sizes[1:1 + 2 * twos:2], sizes[2:2 + 2 * twos:2]
    room = jnp.minimum(source_of - 1, most - taker)
    moved = jax.random.randint(jax.random.fold_in(stream_key, 1), (twos,), 0, 1 << 20) % (room + 1)
    sizes = sizes.at[1:1 + 2 * twos:2].set(source_of - moved).at[2:2 + 2 * twos:2].set(taker + moved)
    return sizes[jax.random.permutation(jax.random.fold_in(stream_key, 2), amount)]


def noise(key, shape, spread, bound, shards=(), kind=jnp.bfloat16):
    values = jax.random.normal(key, shape, jnp.float32) * spread
    if len(shards) > 0:
        values = block_scale(key, shape, shards, -0.22, 0.18) * values
    return jnp.clip(values, min=-bound, max=bound).astype(kind)


def setup_inputs(seed: int = 0) -> dict:
    key_of = jax.random.split(jax.random.key(seed), 8)
    return {
        "queries": draw_queries(jax.random.fold_in(key_of[7], 71), 0),
        "keys": draw_keys(jax.random.fold_in(key_of[7], 71), 0),
        "values": noise(key_of[2], (TOKENS, HEADS * HD), 1.0, 6.0, ((0, 16), (1, 2))),
        "out_weight": noise(key_of[3], (HEADS * HD, D), (HEADS * HD) ** -0.5, 0.125, ((0, 2),)),
        "mixed_grad": noise(key_of[4], (TOKENS, D), 1.0, 6.0, ((0, 16), (1, 2))),
        "lengths": ragged(key_of[5], DOCS, TOKENS, HALF * MAXD + TOK_DEV, 2).astype(jnp.int32),
        "dilation": plant(jax.random.randint(key_of[6], (HEADS,), 1, MAXD + 1), jax.random.fold_in(key_of[6], 1), 1, MAXD).astype(jnp.int32),
    }


def segment_of(positions, lengths):
    boundary = jnp.cumsum(lengths).astype(jnp.int32)
    return jnp.sum((positions[:, None] >= boundary[None, :]).astype(jnp.int32), axis=1)


def allowed(query_pos, key_pos, query_seg, key_seg, dilation, reach, total):
    offset_grid = query_pos[:, None] - key_pos[None, :]
    common = (query_seg[:, None] == key_seg[None, :]) & (key_pos[None, :] >= 0) & (key_pos[None, :] < total)
    common = common & (query_pos[:, None] >= 0) & (query_pos[:, None] < total)
    stride = dilation[:, None, None]
    within = (jnp.abs(offset_grid)[None] <= reach * stride) & (jnp.remainder(offset_grid[None], stride) == 0)
    return within & common[None]


def reference(queries, keys, values, out_weight, mixed_grad, lengths, dilation):
    total = queries.shape[0]
    margin = HALF * MAXD
    factor = HD ** -0.5
    window = TOK_DEV + 2 * margin
    blocks = total // TOK_DEV
    grad_attention = jnp.dot(mixed_grad, out_weight.T, preferred_element_type=jnp.float32).astype(jnp.bfloat16)

    def by_head(array):
        return array.reshape(total, HEADS, HD).transpose(1, 0, 2)

    def one_head(item):
        query_rows, key_rows, value_rows, grad_rows, spacing = item
        padding = ((margin, margin), (0, 0))
        key_padded = jnp.pad(key_rows, padding)
        value_padded = jnp.pad(value_rows, padding)
        zeros_pad = jnp.zeros((total + 2 * margin, HD), jnp.float32)

        def step(carry, block):
            key_acc, value_acc = carry
            start = (block * TOK_DEV).astype(jnp.int32)
            query_block = lax.dynamic_slice_in_dim(query_rows, start, TOK_DEV, 0)
            grad_block = lax.dynamic_slice_in_dim(grad_rows, start, TOK_DEV, 0)
            key_window = lax.dynamic_slice_in_dim(key_padded, start, window, 0)
            value_window = lax.dynamic_slice_in_dim(value_padded, start, window, 0)
            query_pos = start + jnp.arange(TOK_DEV, dtype=jnp.int32)
            key_pos = start - margin + jnp.arange(window, dtype=jnp.int32)
            mask = allowed(query_pos, key_pos, segment_of(query_pos, lengths), segment_of(key_pos, lengths), spacing[None], HALF, total)[0]
            scores = jnp.dot(query_block, key_window.T, preferred_element_type=jnp.float32) * factor
            top = jnp.max(jnp.where(mask, scores, -jnp.inf), axis=1)
            log_total = top + jnp.log(jnp.sum(jnp.where(mask, jnp.exp(scores - top[:, None]), 0.0), axis=1))
            weights = jnp.where(mask, jnp.exp(scores - log_total[:, None]), 0.0)
            probs = weights.astype(jnp.bfloat16)
            attention = jnp.dot(probs, value_window, preferred_element_type=jnp.float32).astype(jnp.bfloat16)
            delta = jnp.sum(grad_block.astype(jnp.float32) * attention.astype(jnp.float32), axis=1)
            grad_prob = jnp.dot(grad_block, value_window.T, preferred_element_type=jnp.float32)
            slopes = (weights * (grad_prob - delta[:, None])).astype(jnp.bfloat16)
            grad_query = (jnp.dot(slopes, key_window, preferred_element_type=jnp.float32) * factor).astype(jnp.bfloat16)
            key_term = jnp.dot(slopes.T, query_block, preferred_element_type=jnp.float32) * factor
            value_term = jnp.dot(probs.T, grad_block, preferred_element_type=jnp.float32)
            key_acc = lax.dynamic_update_slice_in_dim(key_acc, lax.dynamic_slice_in_dim(key_acc, start, window, 0) + key_term, start, 0)
            value_acc = lax.dynamic_update_slice_in_dim(value_acc, lax.dynamic_slice_in_dim(value_acc, start, window, 0) + value_term, start, 0)
            return (key_acc, value_acc), (attention, grad_query)

        (key_acc, value_acc), (attention, grad_query) = lax.scan(step, (zeros_pad, zeros_pad), jnp.arange(blocks, dtype=jnp.int32))
        grad_key = key_acc[margin:margin + total].astype(jnp.bfloat16)
        grad_value = value_acc[margin:margin + total].astype(jnp.bfloat16)
        return attention.reshape(total, HD), grad_query.reshape(total, HD), grad_key, grad_value

    results = lax.map(one_head, (by_head(queries), by_head(keys), by_head(values), by_head(grad_attention), dilation))

    def flat(array):
        return array.transpose(1, 0, 2).reshape(total, HEADS * HD)

    attention = flat(results[0])
    mixed = jnp.dot(attention, out_weight, preferred_element_type=jnp.float32).astype(jnp.bfloat16)
    return mixed, flat(results[1]), flat(results[2]), flat(results[3])
```

```python
import functools
import jax
import jax.numpy as jnp
from jax import lax
from jax.experimental import pallas as pl
from jax.experimental.pallas import tpu as pltpu
from jax.sharding import PartitionSpec as P

HALF = 32
MAXD = 8
FAR = 1e6
NEG = -1e30
HEAD_WIDTH = 128

GROUP = 4
NT = (((1,), (1,)), ((), ()))
TN = (((0,), (0,)), ((), ()))
F32 = jnp.float32
BF16 = jnp.bfloat16
MESH_ID = pl.DeviceIdType.MESH


def fused_kernel(
    groups, length_ref, dilation_ref, q_ref, k_ref, v_ref, w_ref, mg_ref,
    mixed_ref, gq_ref, gk_ref, gv_ref,
    w_own, w_oth, mg_own, mg_oth, kv, qs, gos, go_acc, go_bf, att_my, att_in,
    part_send, part_recv, part_own, probs, spaced, bounds, terms,
    halo_send, halo_recv, dq, dkv,
    w_sem, mg_loc, own_sem, x_send, x_recv, in_send, in_recv, kv_send, kv_recv,
    go_send, go_recv, att_send, att_recv, p_send, p_recv, h_send, h_recv,
    out_send, out_recv, out_loc,
):
    rows = q_ref.shape[0]
    width = HEAD_WIDTH
    lane = q_ref.shape[1] // GROUP
    heads = lane // width
    feats = mg_ref.shape[1]
    chunks = mg_oth.shape[0]
    step = feats // chunks
    window = kv.shape[1] - 2 * rows
    block = 2 * rows
    halo = 2 * rows
    factor = width ** (-0.5)

    c = lax.axis_index("ctx")
    side = lax.axis_index("head")
    g = c // GROUP
    r = c % GROUP
    y = r // 2
    core = r % 2
    peers = (r, r + 1 - 2 * core, r + 2 - 4 * y, (GROUP - 1) - r)
    base = g * GROUP
    ahead = 2 * y - 1
    has_fwd = (g + ahead >= 0) & (g + ahead < groups)
    has_bwd = (g - ahead >= 0) & (g - ahead < groups)
    fwd_id = {"ctx": c + GROUP * ahead}
    bwd_id = {"ctx": c - GROUP * ahead}
    x_id = {"head": 1 - side}

    def peer_id(o):
        return {"ctx": base + peers[o]}

    def lanes(i):
        return pl.ds(pl.multiple_of(i * lane, lane), lane)

    def slab(i, first=0):
        return pl.ds(pl.multiple_of(first + i * rows, rows), rows)

    def remote(src, dst, send, recv, device):
        return pltpu.make_async_remote_copy(
            src_ref=src, dst_ref=dst, send_sem=send, recv_sem=recv,
            device_id=device, device_id_type=MESH_ID,
        )

    def w_copy(half, n):
        where = side if half == 0 else 1 - side
        dst = (w_own, w_oth)[half]
        return pltpu.make_async_copy(
            w_ref.at[:, pl.ds(pl.multiple_of(where * feats + n * step, step), step)],
            dst.at[n], w_sem.at[half, n],
        )

    mg_copy = pltpu.make_async_copy(mg_ref, mg_own, mg_loc)
    own = (
        pltpu.make_async_copy(k_ref.at[:, lanes(r)], kv.at[0, slab(r, halo), :], own_sem.at[0]),
        pltpu.make_async_copy(v_ref.at[:, lanes(r)], kv.at[1, slab(r, halo), :], own_sem.at[1]),
        pltpu.make_async_copy(q_ref.at[:, lanes(r)], qs.at[slab(r), :], own_sem.at[2]),
    )
    own[0].start()
    own[1].start()
    mg_copy.start()
    own[2].start()
    for n in range(chunks):
        w_copy(0, n).start()
    for n in range(chunks):
        w_copy(1, n).start()

    barrier = pltpu.get_barrier_semaphore()
    for o in (1, 2, 3):
        pl.semaphore_signal(barrier, inc=1, device_id=peer_id(o), device_id_type=MESH_ID)
    pl.semaphore_signal(barrier, inc=1, device_id=x_id, device_id_type=MESH_ID)

    @pl.when(has_fwd)
    def _():
        pl.semaphore_signal(barrier, inc=1, device_id=fwd_id, device_id_type=MESH_ID)

    @pl.when(has_bwd)
    def _():
        pl.semaphore_signal(barrier, inc=1, device_id=bwd_id, device_id_type=MESH_ID)

    neighbours = has_fwd.astype(jnp.int32) + has_bwd.astype(jnp.int32)
    pl.semaphore_wait(barrier, GROUP + neighbours)

    def x_copy(n):
        return remote(
            mg_ref.at[:, pl.ds(n * step, step)], mg_oth.at[n], x_send.at[n], x_recv.at[n], x_id
        )

    def in_copy(t, o):
        source = (k_ref, v_ref, q_ref)[t].at[:, lanes(peers[o])]
        dst = kv.at[t, slab(r, halo), :] if t < 2 else qs.at[slab(r), :]
        return remote(source, dst, in_send.at[t, o], in_recv.at[t, o], peer_id(o))

    for t, o in ((0, 1), (1, 1), (0, 2), (1, 2), (0, 3), (1, 3), (2, 2), (2, 3), (2, 1)):
        in_copy(t, o).start()
    for n in range(chunks):
        x_copy(n).start()

    def relay(o):
        to = ahead if o < 2 else -ahead
        src_row = halo + peers[o] * rows
        dst_row = src_row - to * (GROUP * rows)
        return remote(
            kv.at[:, pl.ds(pl.multiple_of(src_row, rows), rows), :],
            kv.at[:, pl.ds(pl.multiple_of(dst_row, rows), rows), :],
            kv_send.at[o], kv_recv.at[o], fwd_id if o < 2 else bwd_id,
        )

    rel = lax.broadcasted_iota(jnp.int32, (window, block), 0) - halo
    rel = rel - lax.broadcasted_iota(jnp.int32, (window, block), 1)
    relf = rel.astype(F32)
    for h in range(heads):
        spacing = jnp.full((1, block), dilation_ref[r * heads + h], jnp.int32)
        inv = 1.0 / spacing.astype(F32)
        steps = relf * inv
        whole = jnp.floor(steps + 0.5)
        spaced[h] = jnp.where(jnp.abs(steps - whole) < 0.01, rel, 1 << 24)
    for b in range(2):
        qpos = base * rows + b * block + lax.broadcasted_iota(jnp.int32, (1, block), 1)
        start = jnp.zeros((1, block), jnp.int32)
        stop = jnp.full((1, block), 1 << 24, jnp.int32)
        end = jnp.int32(0)
        for n in range(length_ref.shape[0]):
            end = end + length_ref[n]
            past = qpos >= end
            start = jnp.where(past, jnp.maximum(start, end), start)
            stop = jnp.where(past, stop, jnp.minimum(stop, end))
        for h in range(heads):
            reach = jnp.full((1, block), HALF * dilation_ref[r * heads + h], jnp.int32)
            bounds[b, h, 0:1, :] = jnp.maximum(start - qpos, -reach)
            bounds[b, h, 1:2, :] = jnp.minimum(stop - 1 - qpos, reach)

    near_row = pl.multiple_of((halo + GROUP * rows) * (1 - y), halo)
    far_row = pl.multiple_of((halo + GROUP * rows) * y, halo)

    @pl.when(jnp.logical_not(has_bwd))
    def _():
        kv[:, pl.ds(near_row, halo), :] = jnp.zeros((2, halo, lane), BF16)
        halo_recv[1] = jnp.zeros(halo_recv.shape[1:], BF16)

    @pl.when(jnp.logical_not(has_fwd))
    def _():
        kv[:, pl.ds(far_row, halo), :] = jnp.zeros((2, halo, lane), BF16)
        halo_recv[0] = jnp.zeros(halo_recv.shape[1:], BF16)

    own[0].wait()
    own[1].wait()

    @pl.when(has_fwd)
    def _():
        relay(0).start()

    def go_step(mg, weight, first):
        term = lax.dot_general(mg, weight, NT, preferred_element_type=F32)
        if first:
            go_acc[...] = term
        else:
            go_acc[...] += term

    mg_copy.wait()
    for n in range(chunks):
        w_copy(0, n).wait()
        go_step(mg_own[:, n * step : (n + 1) * step], w_own[n], n == 0)
        if n == 0:
            for t in (0, 1):
                in_copy(t, 1).wait_recv()

            @pl.when(has_fwd)
            def _():
                relay(1).start()

    for o in (2, 3):
        for t in (0, 1):
            in_copy(t, o).wait_recv()

        @pl.when(has_bwd)
        def _():
            relay(o).start()

    def go_far(n):
        w_copy(1, n).wait()
        x_copy(n).wait_recv()
        go_step(mg_oth[n], w_oth[n], False)

    for n in range(chunks // 2):
        go_far(n)

    for o in (2, 3, 1):
        in_copy(2, o).wait_recv()
    own[2].wait()

    def at_rows(i):
        return pl.multiple_of((1 - y) * block if i == 0 else y * block, block)

    def forward(i, h):
        row0 = at_rows(i)
        col = slice(h * width, (h + 1) * width)
        b = 1 - y if i == 0 else y
        k = kv[0, pl.ds(row0, window), col]
        v = kv[1, pl.ds(row0, window), col]
        q = qs[pl.ds(row0, block), col]
        s = lax.dot_general(k, q, NT, preferred_element_type=F32)
        rel = spaced[h]
        lo = bounds[b, h, 0:1, :]
        hi = bounds[b, h, 1:2, :]
        s = jnp.where((rel >= lo) & (rel <= hi), s, NEG)
        top = jnp.max(s, axis=0, keepdims=True)
        e = jnp.exp((s - top) * factor)
        w = e * (1.0 / jnp.sum(e, axis=0, keepdims=True))
        p = w.astype(BF16)
        probs[i, h] = p
        att = lax.dot_general(p, v, TN, preferred_element_type=F32)
        att_my[pl.ds(row0, block), col] = att.astype(BF16)

    def att_copy(o):
        return remote(
            att_my.at[slab(peers[o]), :], att_in.at[:, lanes(r)],
            att_send.at[o], att_recv.at[o], peer_id(o),
        )

    att_local = pltpu.make_async_copy(att_my.at[slab(r), :], att_in.at[:, lanes(r)], own_sem.at[3])

    for o in (0, 1):
        @pl.when(has_bwd)
        def _():
            relay(o).wait_recv()
    for h in range(heads):
        forward(0, h)
    for o in (2, 3):
        att_copy(o).start()
    for o in (2, 3):
        @pl.when(has_fwd)
        def _():
            relay(o).wait_recv()
    for h in range(heads):
        forward(1, h)
    att_copy(1).start()
    att_local.start()

    for n in range(chunks // 2, chunks):
        go_far(n)
    go_bf[...] = go_acc[...].astype(BF16)

    def go_copy(o):
        return remote(
            go_bf.at[:, lanes(peers[o])], gos.at[slab(r), :],
            go_send.at[o], go_recv.at[o], peer_id(o),
        )

    go_local = pltpu.make_async_copy(go_bf.at[:, lanes(r)], gos.at[slab(r), :], own_sem.at[4])
    for o in (2, 3, 1):
        go_copy(o).start()
    go_local.start()

    att_local.wait()
    for o in (1, 2, 3):
        att_copy(o).wait_recv()

    def p_copy(n):
        return remote(part_send.at[n], part_recv.at[n], p_send.at[n], p_recv.at[n], x_id)

    for n in range(chunks):
        part = jnp.dot(att_in[...], w_oth[n], preferred_element_type=F32)
        part_send[n] = part.astype(BF16)
        p_copy(n).start()

    go_local.wait()
    for o in (1, 2, 3):
        go_copy(o).wait_recv()

    def backward(i, h):
        row0 = at_rows(i)
        col = slice(h * width, (h + 1) * width)
        k = kv[0, pl.ds(row0, window), col]
        v = kv[1, pl.ds(row0, window), col]
        q = qs[pl.ds(row0, block), col]
        go = gos[pl.ds(row0, block), col]
        gp = lax.dot_general(v, go, NT, preferred_element_type=F32)
        p = probs[i, h]
        w = p.astype(F32)
        delta = jnp.sum(w * gp, axis=0, keepdims=True)
        s = (w * (gp - delta)).astype(BF16)
        terms[i, h, 0] = jnp.dot(s, q, preferred_element_type=F32) * factor
        terms[i, h, 1] = jnp.dot(p, go, preferred_element_type=F32)
        edge = pl.ds(pl.multiple_of(2 * row0, block), block)
        for t in range(2):
            halo_send[i, h, t] = terms[i, h, t, edge, :].astype(BF16)
        gq = lax.dot_general(s, k, TN, preferred_element_type=F32) * factor
        dq[pl.ds(row0, block), col] = gq.astype(BF16)

    def h_copy(i, h):
        return remote(
            halo_send.at[i, h], halo_recv.at[i, h], h_send.at[i, h], h_recv.at[i, h],
            bwd_id if i == 0 else fwd_id,
        )

    for h in range(heads):
        backward(0, h)

        @pl.when(has_bwd)
        def _():
            h_copy(0, h).start()

        backward(1, h)

        @pl.when(has_fwd)
        def _():
            h_copy(1, h).start()

    def dq_copy(o):
        return remote(
            dq.at[slab(peers[o]), :], gq_ref.at[:, lanes(r)],
            out_send.at[0, o], out_recv.at[0, o], peer_id(o),
        )

    dq_local = pltpu.make_async_copy(dq.at[slab(r), :], gq_ref.at[:, lanes(r)], out_loc.at[0])
    for o in (2, 3, 1):
        dq_copy(o).start()
    dq_local.start()

    for n in range(chunks):
        part_own[n] = jnp.dot(att_in[...], w_own[n], preferred_element_type=F32)

    for h in range(heads):
        @pl.when(has_fwd)
        def _():
            h_copy(0, h).wait_recv()

        @pl.when(has_bwd)
        def _():
            h_copy(1, h).wait_recv()

        for i in range(2):
            half = y * block if i == 0 else (1 - y) * block
            out = pl.ds(pl.multiple_of(half, block), block)
            first = pl.ds(pl.multiple_of(half + halo - at_rows(0), block), block)
            second = pl.ds(pl.multiple_of(half + halo - at_rows(1), block), block)
            for t in range(2):
                total = terms[0, h, t, first, :] + terms[1, h, t, second, :]
                total = total + halo_recv[i, h, t].astype(F32)
                dkv[t, out, h * width : (h + 1) * width] = total.astype(BF16)

    def dkv_copy(t, o):
        return remote(
            dkv.at[t, slab(peers[o]), :], (gk_ref, gv_ref)[t].at[:, lanes(r)],
            out_send.at[1 + t, o], out_recv.at[1 + t, o], peer_id(o),
        )

    def dkv_local(t):
        return pltpu.make_async_copy(
            dkv.at[t, slab(r), :], (gk_ref, gv_ref)[t].at[:, lanes(r)], out_loc.at[1 + t]
        )

    for o in (2, 3, 1):
        for t in range(2):
            dkv_copy(t, o).start()
    for t in range(2):
        dkv_local(t).start()

    for n in range(chunks):
        p_copy(n).wait_recv()
        total = part_own[n] + part_recv[n].astype(F32)
        mixed_ref[:, n * step : (n + 1) * step] = total.astype(BF16)

    for o in (1, 2, 3):
        for t in range(3):
            in_copy(t, o).wait_send()
        att_copy(o).wait_send()
        go_copy(o).wait_send()
        dq_copy(o).wait()
        for t in range(2):
            dkv_copy(t, o).wait()
    for n in range(chunks):
        x_copy(n).wait_send()
        p_copy(n).wait_send()

    @pl.when(has_fwd)
    def _():
        for o in (0, 1):
            relay(o).wait_send()
        for h in range(heads):
            h_copy(1, h).wait_send()

    @pl.when(has_bwd)
    def _():
        for o in (2, 3):
            relay(o).wait_send()
        for h in range(heads):
            h_copy(0, h).wait_send()

    dq_local.wait()
    for t in range(2):
        dkv_local(t).wait()


def fused(queries, keys, values, out_weight, mixed_grad, lengths, dilation, groups, chunks=4):
    rows, cols = queries.shape
    lane = cols // GROUP
    width = HEAD_WIDTH
    heads = lane // width
    feats = mixed_grad.shape[1]
    step = feats // chunks
    block, halo, tokens = 2 * rows, 2 * rows, GROUP * rows
    window = block + 2 * halo
    smem = pl.BlockSpec(memory_space=pltpu.SMEM)
    hbm = pl.BlockSpec(memory_space=pl.ANY)
    vmem = pl.BlockSpec(memory_space=pltpu.VMEM)
    dma = pltpu.SemaphoreType.DMA
    V = pltpu.VMEM
    one = jax.ShapeDtypeStruct((rows, cols), BF16)
    return pl.pallas_call(
        functools.partial(fused_kernel, groups),
        in_specs=[smem, smem, hbm, hbm, hbm, hbm, hbm],
        out_specs=[vmem] * 4,
        out_shape=[jax.ShapeDtypeStruct((rows, feats), BF16), one, one, one],
        scratch_shapes=[
            V((chunks, cols, step), BF16), V((chunks, cols, step), BF16),
            V((rows, feats), BF16), V((chunks, rows, step), BF16),
            V((2, tokens + 2 * halo, lane), BF16), V((tokens, lane), BF16), V((tokens, lane), BF16),
            V((rows, cols), F32), V((rows, cols), BF16), V((tokens, lane), BF16), V((rows, cols), BF16),
            V((chunks, rows, step), BF16), V((chunks, rows, step), BF16), V((chunks, rows, step), F32),
            V((2, heads, window, block), BF16), V((heads, window, block), jnp.int32),
            V((2, heads, 8, block), jnp.int32), V((2, heads, 2, window, width), F32),
            V((2, heads, 2, halo, width), BF16), V((2, heads, 2, halo, width), BF16),
            V((tokens, lane), BF16), V((2, tokens, lane), BF16),
            dma((2, chunks)), dma, dma((5,)), dma((chunks,)), dma((chunks,)),
            dma((3, GROUP)), dma((3, GROUP)), dma((GROUP,)), dma((GROUP,)),
            dma((GROUP,)), dma((GROUP,)), dma((GROUP,)), dma((GROUP,)),
            dma((chunks,)), dma((chunks,)), dma((2, heads)), dma((2, heads)),
            dma((3, GROUP)), dma((3, GROUP)), dma((3,)),
        ],
        compiler_params=pltpu.CompilerParams(
            collective_id=0, has_side_effects=True, vmem_limit_bytes=60000 * 1024
        ),
    )(lengths, dilation, queries, keys, values, out_weight, mixed_grad)


def attend_kernel(
    row_count, total, factor, first, index_ref, length_ref, dilation_ref,
    q_ref, go_ref, own_ref, a_ref, b_ref, po_ref, pa_ref,
    att_ref, gq_ref, own_t, a_t, b_t, po_t, pa_t, dist,
):
    slabs = (own_ref, a_ref, b_ref, po_ref, pa_ref)
    outs = (own_t, a_t, b_t, po_t, pa_t)

    @pl.when(pl.program_id(0) == 0)
    def _():
        me = index_ref[0]
        sign = 1 - 2 * lax.rem(me, 2)
        ends = [length_ref[0]]
        for n in range(1, length_ref.shape[0]):
            ends.append(ends[-1] + length_ref[n])

        def segment(pos):
            seg = jnp.zeros(pos.shape, jnp.int32)
            for end in ends:
                seg = seg + (pos >= end).astype(jnp.int32)
            return seg

        qpos = me * row_count + lax.broadcasted_iota(jnp.int32, (1, row_count), 1)
        qseg = segment(qpos)
        for i, off in enumerate((0, 2, -2, 1, -1)):
            kpos = (me + sign * off) * row_count + lax.broadcasted_iota(
                jnp.int32, (row_count, row_count), 0
            )
            same = (segment(kpos) == qseg) & (kpos >= 0) & (kpos < total)
            gap = jnp.abs(kpos - qpos).astype(jnp.float32)
            dist[pl.ds(i * row_count, row_count), :] = jnp.where(same, gap, FAR)

    spacing = jnp.full((1, row_count), dilation_ref[first + pl.program_id(0)], jnp.int32)
    inv = 1.0 / spacing.astype(jnp.float32)
    steps = dist[...] * inv
    whole = jnp.floor(steps + 0.5)
    mask = (whole <= HALF) & (jnp.abs(steps - whole) < 0.01)
    q = q_ref[...]
    go = go_ref[...]
    k = jnp.concatenate([r[0] for r in slabs], axis=0)
    v = jnp.concatenate([r[1] for r in slabs], axis=0)
    nt = (((1,), (1,)), ((), ()))
    tn = (((0,), (0,)), ((), ()))
    f32 = jnp.float32
    scores = lax.dot_general(k, q, nt, preferred_element_type=f32) * factor
    scores = jnp.where(mask, scores, NEG)
    top = jnp.max(scores, axis=0, keepdims=True)
    e = jnp.exp(scores - top)
    w = e * (1.0 / jnp.sum(e, axis=0, keepdims=True))
    p = w.astype(jnp.bfloat16)
    gp = lax.dot_general(v, go, nt, preferred_element_type=f32)
    delta = jnp.sum(w * gp, axis=0, keepdims=True)
    s = (w * (gp - delta)).astype(jnp.bfloat16)
    att_ref[...] = lax.dot_general(p, v, tn, preferred_element_type=f32).astype(jnp.bfloat16)
    gq_ref[...] = (
        lax.dot_general(s, k, tn, preferred_element_type=f32) * factor
    ).astype(jnp.bfloat16)
    kt = (jnp.dot(s, q, preferred_element_type=f32) * factor).astype(jnp.bfloat16)
    vt = jnp.dot(p, go, preferred_element_type=f32).astype(jnp.bfloat16)
    for i, out in enumerate(outs):
        out[0] = kt[i * row_count : (i + 1) * row_count]
        out[1] = vt[i * row_count : (i + 1) * row_count]


def attend(index, lengths, dilation, q, go, slabs, first, total, factor, width):
    rows, cols = q.shape[0], slabs[0].shape[2]
    heads = cols // width
    smem = pl.BlockSpec(memory_space=pltpu.SMEM)
    shared = pl.BlockSpec((rows, width), lambda h: (0, first + h))
    flat = pl.BlockSpec((rows, width), lambda h: (0, h))
    pair = pl.BlockSpec((2, rows, width), lambda h: (0, 0, h))
    one = jax.ShapeDtypeStruct((rows, cols), jnp.bfloat16)
    two = jax.ShapeDtypeStruct((2, rows, cols), jnp.bfloat16)
    return pl.pallas_call(
        functools.partial(attend_kernel, rows, total, factor, first),
        grid=(heads,),
        in_specs=[smem, smem, smem, shared, shared] + [pair] * 5,
        out_specs=[flat, flat] + [pair] * 5,
        out_shape=[one, one] + [two] * 5,
        scratch_shapes=[pltpu.VMEM((5 * rows, rows), jnp.float32)],
        compiler_params=pltpu.CompilerParams(dimension_semantics=("arbitrary",)),
        cost_estimate=pl.CostEstimate(
            flops=heads * 6 * 2 * 5 * rows * rows * width * 8,
            bytes_accessed=24 * 2 * rows * cols,
            transcendentals=heads * 5 * rows * rows,
        ),
    )(index, lengths, dilation, q, go, *slabs)


def per_device(queries, keys, values, out_weight, mixed_grad, lengths, dilation):
    rows = queries.shape[0]
    local_heads = dilation.shape[0]
    width = queries.shape[1] // local_heads
    factor = width ** (-0.5)
    count = lax.axis_size("ctx")
    sides = lax.axis_size("head")
    total = rows * count
    assert 2 * rows >= HALF * MAXD and count % 2 == 0
    if sides == 2 and count % GROUP == 0 and local_heads % GROUP == 0 and width == HEAD_WIDTH:
        if 2 * rows == HALF * MAXD and mixed_grad.shape[1] % 512 == 0:
            return fused(
                queries, keys, values, out_weight, mixed_grad, lengths, dilation, count // GROUP
            )
    index = lax.axis_index("ctx").astype(jnp.int32).reshape(1)

    inward = [
        (j, t) for j in range(count) for t in [j - 2 if j % 2 == 0 else j + 2] if 0 <= t < count
    ]
    outward = [(t, j) for j, t in inward]
    swapped = [(j, j ^ 1) for j in range(count)]

    def move(x, pairs):
        return lax.ppermute(x, "ctx", pairs)

    groups = 1
    gh = local_heads // groups
    cut = [slice(g * gh * width, (g + 1) * gh * width) for g in range(groups)]
    half = mixed_grad.shape[1]
    if sides == 2:
        other = lax.ppermute(mixed_grad, "head", [(0, 1), (1, 0)])
        left = lax.axis_index("head") == 0
        grad_full = jnp.concatenate(
            [jnp.where(left, mixed_grad, other), jnp.where(left, other, mixed_grad)], axis=1
        )
    else:
        grad_full = lax.all_gather(mixed_grad, "head", axis=1, tiled=True)
    stacks = []
    for g in range(groups):
        own = jnp.stack([keys[:, cut[g]], values[:, cut[g]]])
        stacks.append([own, move(own, inward), move(own, outward), move(own, swapped)])
    grad_attention = lax.dot_general(
        grad_full, out_weight, (((1,), (1,)), ((), ())), preferred_element_type=jnp.float32
    ).astype(jnp.bfloat16)

    atts, gqs, gkvs = [], [], []
    f32 = jnp.float32
    for slabs in stacks:
        slabs[1], grad_attention = lax.optimization_barrier((slabs[1], grad_attention))
        slabs.append(move(slabs[1], swapped))
    for g in range(groups):
        att, gq, own_t, a_t, b_t, po_t, pa_t = attend(
            index, lengths, dilation, queries, grad_attention, stacks[g], g * gh, total, factor, width
        )
        pa_back = move(pa_t, swapped)
        b_back = move(b_t, inward)
        po_back = move(po_t, swapped)
        a_sum = (a_t.astype(f32) + pa_back.astype(f32)).astype(jnp.bfloat16)
        a_sum, att = lax.optimization_barrier((a_sum, att))
        a_back = move(a_sum, outward)
        terms = (own_t, po_back, b_back, a_back)
        gkvs.append(
            [sum(term[i].astype(f32) for term in terms).astype(jnp.bfloat16) for i in range(2)]
        )
        atts.append(att)
        gqs.append(gq)
    attention = jnp.concatenate(atts, axis=1)
    partial = jnp.dot(attention, out_weight, preferred_element_type=f32)
    if sides == 2:
        lo, hi = partial[:, :half], partial[:, half:]
        away = jnp.where(left, hi, lo).astype(jnp.bfloat16)
        came = lax.ppermute(away, "head", [(0, 1), (1, 0)])
        mixed = (jnp.where(left, lo, hi) + came.astype(f32)).astype(jnp.bfloat16)
    else:
        mixed = lax.psum_scatter(
            partial.astype(jnp.bfloat16), "head", scatter_dimension=1, tiled=True
        )
    grad_keys, grad_values = (
        jnp.concatenate([pair[i] for pair in gkvs], axis=1) for i in range(2)
    )
    return mixed, jnp.concatenate(gqs, axis=1), grad_keys, grad_values


def solution(mesh):
    both = P("ctx", "head")
    return jax.shard_map(
        per_device,
        mesh=mesh,
        in_specs=(both, both, both, P("head", None), both, P(), P("head")),
        out_specs=(both, both, both, both),
        check_vma=False,
    )
```

```python
import functools
import jax
import jax.numpy as jnp
from jax import lax
from jax.experimental import pallas as pl
from jax.experimental.pallas import tpu as pltpu
from jax.sharding import PartitionSpec as P

HALF = 32
MAXD = 8
FAR = 1e6
NEG = -1e30
HEAD_WIDTH = 128

GROUP = 4
NT = (((1,), (1,)), ((), ()))
TN = (((0,), (0,)), ((), ()))
F32 = jnp.float32
BF16 = jnp.bfloat16
MESH_ID = pl.DeviceIdType.MESH


def fused_kernel(
    groups, length_hbm, dilation_hbm, q_ref, k_ref, v_ref, w_ref, mg_ref,
    mixed_ref, gq_ref, gk_ref, gv_ref,
    w_own, w_oth, mg_own, mg_oth, kv, qs, gos, go_acc, go_bf, att_my, att_in,
    part_send, part_recv, part_own, probs, spaced, bounds, terms,
    slopes, halo_send, halo_recv, dq, dkv, mixed_out, length_ref, dilation_ref,
    int_sem, w_sem, mg_sem, own_sem, x_recv, kv_recv, q_recv, halo_kv, go_recv, att_recv,
    p_recv, h_recv, out_recv, mixed_sem, sent, sent_fwd, sent_bwd,
):
    rows = q_ref.shape[0]
    width = HEAD_WIDTH
    heads = q_ref.shape[1] // GROUP // width
    feats = mg_ref.shape[1]
    chunks = mg_oth.shape[0]
    step = feats // chunks
    window = kv.shape[2] - 2 * rows
    block = 2 * rows
    halo = 2 * rows
    factor = width ** (-0.5)
    scope = jax.named_scope

    c = lax.axis_index("ctx")
    side = lax.axis_index("head")
    g = c // GROUP
    r = c % GROUP
    y = r // 2
    core = r % 2
    peers = (r, r + 1 - 2 * core, r + 2 - 4 * y, (GROUP - 1) - r)
    base = g * GROUP
    ahead = 2 * y - 1
    has_fwd = (g + ahead >= 0) & (g + ahead < groups)
    has_bwd = (g - ahead >= 0) & (g - ahead < groups)
    fwd_id = {"ctx": c + GROUP * ahead}
    bwd_id = {"ctx": c - GROUP * ahead}
    x_id = {"head": 1 - side}

    def peer_id(o):
        return {"ctx": base + peers[o]}

    def lanes(i, h):
        return pl.ds(pl.multiple_of((i * heads + h) * width, width), width)

    def slab(i, first=0):
        return pl.ds(pl.multiple_of(first + i * rows, rows), rows)

    def arrived(ref, sem):
        pltpu.make_async_copy(ref, ref, sem).wait()

    def remote(src, dst, send, recv, device):
        return pltpu.make_async_remote_copy(
            src_ref=src, dst_ref=dst, send_sem=send, recv_sem=recv,
            device_id=device, device_id_type=MESH_ID,
        )

    integers = (
        pltpu.make_async_copy(length_hbm, length_ref, int_sem.at[0]),
        pltpu.make_async_copy(dilation_hbm, dilation_ref, int_sem.at[1]),
    )
    for copy in integers:
        copy.start()

    barrier = pltpu.get_barrier_semaphore()
    for o in (1, 2, 3):
        pl.semaphore_signal(barrier, inc=1, device_id=peer_id(o), device_id_type=MESH_ID)
    pl.semaphore_signal(barrier, inc=1, device_id=x_id, device_id_type=MESH_ID)

    @pl.when(has_fwd)
    def _():
        pl.semaphore_signal(barrier, inc=1, device_id=fwd_id, device_id_type=MESH_ID)

    @pl.when(has_bwd)
    def _():
        pl.semaphore_signal(barrier, inc=1, device_id=bwd_id, device_id_type=MESH_ID)

    def w_copy(half):
        where = side if half == 0 else 1 - side
        return pltpu.make_async_copy(
            w_ref.at[:, pl.ds(pl.multiple_of(where * feats, feats), feats)],
            (w_own, w_oth)[half], w_sem.at[half],
        )

    def part(n):
        return slice(n * step, (n + 1) * step)

    def in_place(t, h):
        return kv.at[h, t, slab(r, halo), :] if t < 2 else qs.at[h, slab(r), :]

    def own(t, h):
        source = (k_ref, v_ref, q_ref)[t].at[:, lanes(r, h)]
        return pltpu.make_async_copy(source, in_place(t, h), own_sem if t < 2 else q_recv.at[h])

    mg_copy = pltpu.make_async_copy(mg_ref, mg_own, mg_sem)
    for h in range(heads):
        own(0, h).start()
        own(1, h).start()
    mg_copy.start()
    w_copy(0).start()
    for h in range(heads):
        own(2, h).start()

    neighbours = has_fwd.astype(jnp.int32) + has_bwd.astype(jnp.int32)
    with scope("barrier"):
        pl.semaphore_wait(barrier, GROUP + neighbours)

    def x_copy(n):
        return remote(
            mg_ref.at[:, pl.ds(n * step, step)], mg_oth.at[n], sent, x_recv.at[n], x_id
        )

    def in_copy(t, o, h):
        source = (k_ref, v_ref, q_ref)[t].at[:, lanes(peers[o], h)]
        recv = kv_recv.at[o - 1, h] if t < 2 else q_recv.at[h]
        return remote(source, in_place(t, h), sent, recv, peer_id(o))

    with scope("send"):
        x_copy(0).start()
        for h in range(heads):
            for t, o in ((0, 2), (1, 2), (0, 3), (1, 3), (0, 1), (1, 1)):
                in_copy(t, o, h).start()
        for n in range(1, chunks):
            x_copy(n).start()
        for h in range(heads):
            for o in (2, 3, 1):
                in_copy(2, o, h).start()
        w_copy(1).start()

    def relay(o, h):
        to = ahead if o < 2 else -ahead
        src_row = halo + peers[o] * rows
        dst_row = src_row - to * (GROUP * rows)
        return remote(
            kv.at[h, :, pl.ds(pl.multiple_of(src_row, rows), rows), :],
            kv.at[h, :, pl.ds(pl.multiple_of(dst_row, rows), rows), :],
            sent_fwd if o < 2 else sent_bwd, halo_kv.at[o // 2, h], fwd_id if o < 2 else bwd_id,
        )

    def pass_on(o, h):
        if o > 0:
            arrived(kv.at[h, :, slab(peers[o], halo), :], kv_recv.at[o - 1, h])

        @pl.when(has_fwd if o < 2 else has_bwd)
        def _():
            relay(o, h).start()

    near_row = pl.multiple_of((halo + GROUP * rows) * (1 - y), halo)
    far_row = pl.multiple_of((halo + GROUP * rows) * y, halo)

    @pl.when(jnp.logical_not(has_bwd))
    def _():
        for h in range(heads):
            kv[h, :, pl.ds(near_row, halo), :] = jnp.zeros((2, halo, width), BF16)
        halo_recv[1] = jnp.zeros(halo_recv.shape[1:], BF16)

    @pl.when(jnp.logical_not(has_fwd))
    def _():
        for h in range(heads):
            kv[h, :, pl.ds(far_row, halo), :] = jnp.zeros((2, halo, width), BF16)
        halo_recv[0] = jnp.zeros(halo_recv.shape[1:], BF16)

    arrived(kv.at[:, :, slab(r, halo), :], own_sem)
    for h in range(heads):
        pass_on(0, h)

    for copy in integers:
        copy.wait()
    with scope("masks"):
        rel = lax.broadcasted_iota(jnp.int32, (window, block), 0) - halo
        rel = rel - lax.broadcasted_iota(jnp.int32, (window, block), 1)
        relf = rel.astype(F32)
        for h in range(heads):
            spacing = jnp.full((1, block), dilation_ref[r * heads + h], jnp.int32)
            inv = 1.0 / spacing.astype(F32)
            steps = relf * inv
            whole = jnp.floor(steps + 0.5)
            spaced[h] = jnp.where(jnp.abs(steps - whole) < 0.01, rel, 1 << 24)
        for b in range(2):
            qpos = base * rows + b * block + lax.broadcasted_iota(jnp.int32, (1, block), 1)
            start = jnp.zeros((1, block), jnp.int32)
            stop = jnp.full((1, block), 1 << 24, jnp.int32)
            end = jnp.int32(0)
            for n in range(length_ref.shape[0]):
                end = end + length_ref[n]
                past = qpos >= end
                start = jnp.where(past, jnp.maximum(start, end), start)
                stop = jnp.where(past, stop, jnp.minimum(stop, end))
            for h in range(heads):
                reach = jnp.full((1, block), HALF * dilation_ref[r * heads + h], jnp.int32)
                bounds[b, h, 0:1, :] = jnp.maximum(start - qpos, -reach)
                bounds[b, h, 1:2, :] = jnp.minimum(stop - 1 - qpos, reach)

    def go_step(mg, weight, first):
        term = lax.dot_general(mg, weight, NT, preferred_element_type=F32)
        if first:
            go_acc[...] = term
        else:
            go_acc[...] += term

    mg_copy.wait()
    w_copy(0).wait()
    for n in range(chunks):
        with scope("go_own"):
            go_step(mg_own[:, part(n)], w_own[:, part(n)], n == 0)

    def go_far(n):
        if n == 0:
            w_copy(1).wait()
        with scope("wait_x"):
            x_copy(n).wait_recv()
        with scope("go_far"):
            go_step(mg_oth[n], w_oth[:, part(n)], False)

    with scope("wait_kv"):
        for h in range(heads):
            pass_on(1, h)
        for h in range(heads):
            for o in (2, 3):
                pass_on(o, h)

    def at_rows(i):
        return pl.multiple_of((1 - y) * block if i == 0 else y * block, block)

    def forward(i, h):
        row0 = at_rows(i)
        b = 1 - y if i == 0 else y
        k = kv[h, 0, pl.ds(row0, window), :]
        v = kv[h, 1, pl.ds(row0, window), :]
        q = qs[h, pl.ds(row0, block), :]
        s = lax.dot_general(k, q, NT, preferred_element_type=F32)
        rel = spaced[h]
        lo = bounds[b, h, 0:1, :]
        hi = bounds[b, h, 1:2, :]
        s = jnp.where((rel >= lo) & (rel <= hi), s, NEG)
        top = jnp.max(s, axis=0, keepdims=True)
        e = jnp.exp((s - top) * factor)
        w = e * (1.0 / jnp.sum(e, axis=0, keepdims=True))
        p = w.astype(BF16)
        probs[i, h] = p
        att = lax.dot_general(p, v, TN, preferred_element_type=F32)
        att_my[h, pl.ds(row0, block), :] = att.astype(BF16)

    def att_copy(o, h):
        return remote(
            att_my.at[h, slab(peers[o]), :], att_in.at[:, lanes(r, h)],
            sent, att_recv, peer_id(o),
        )

    def att_local(h):
        return pltpu.make_async_copy(
            att_my.at[h, slab(r), :], att_in.at[:, lanes(r, h)], att_recv
        )

    def near_block(h):
        with scope("wait_q"):
            arrived(qs.at[h], q_recv.at[h])

        @pl.when(has_bwd)
        def _():
            with scope("wait_near"):
                arrived(kv.at[h, :, pl.ds(near_row, halo), :], halo_kv.at[0, h])

        with scope("forward"):
            forward(0, h)
        for o in (2, 3):
            att_copy(o, h).start()

    def far_block(h):
        @pl.when(has_fwd)
        def _():
            with scope("wait_far"):
                arrived(kv.at[h, :, pl.ds(far_row, halo), :], halo_kv.at[1, h])

        with scope("forward"):
            forward(1, h)
        att_copy(1, h).start()
        att_local(h).start()

    go_far(0)
    for h in range(heads):
        near_block(h)
        far_block(h)
    for n in range(1, chunks):
        go_far(n)

    def go_copy(o, h):
        return remote(
            go_bf.at[:, lanes(peers[o], h)], gos.at[h, slab(r), :],
            sent, go_recv.at[h], peer_id(o),
        )

    def go_local(h):
        return pltpu.make_async_copy(go_bf.at[:, lanes(r, h)], gos.at[h, slab(r), :], go_recv.at[h])

    go_bf[...] = go_acc[...].astype(BF16)
    for h in range(heads):
        for o in (2, 3, 1):
            go_copy(o, h).start()
        go_local(h).start()

    with scope("wait_att"):
        arrived(att_in, att_recv)

    def p_copy(n):
        return remote(part_send.at[n], part_recv.at[n], sent, p_recv.at[n], x_id)

    for n in range(chunks):
        with scope("proj_far"):
            term = jnp.dot(att_in[...], w_oth[:, part(n)], preferred_element_type=F32)
            part_send[n] = term.astype(BF16)
        p_copy(n).start()

    with scope("proj_own"):
        for n in range(chunks):
            part_own[n] = jnp.dot(att_in[...], w_own[:, part(n)], preferred_element_type=F32)

    def edge_rows(i):
        return pl.ds(pl.multiple_of(2 * at_rows(i), block), block)

    def edge_values(i, h):
        go = gos[h, pl.ds(at_rows(i), block), :]
        dv = jnp.dot(probs[i, h, edge_rows(i), :], go, preferred_element_type=F32)
        halo_send[i, h, 1] = dv.astype(BF16)

    def edge_keys(i, h):
        row0 = at_rows(i)
        v = kv[h, 1, pl.ds(row0, window), :]
        q = qs[h, pl.ds(row0, block), :]
        go = gos[h, pl.ds(row0, block), :]
        gp = lax.dot_general(v, go, NT, preferred_element_type=F32)
        w = probs[i, h].astype(F32)
        delta = jnp.sum(w * gp, axis=0, keepdims=True)
        slopes[i, h] = (w * (gp - delta)).astype(BF16)
        dk = jnp.dot(slopes[i, h, edge_rows(i), :], q, preferred_element_type=F32) * factor
        halo_send[i, h, 0] = dk.astype(BF16)

    def query_terms(i, h):
        row0 = at_rows(i)
        k = kv[h, 0, pl.ds(row0, window), :]
        gq = lax.dot_general(slopes[i, h], k, TN, preferred_element_type=F32) * factor
        dq[h, pl.ds(row0, block), :] = gq.astype(BF16)

    def inner_terms(i, h):
        row0 = at_rows(i)
        q = qs[h, pl.ds(row0, block), :]
        go = gos[h, pl.ds(row0, block), :]
        inner = pl.ds(pl.multiple_of(halo - row0, block), 2 * block)
        terms[i, h, 0] = jnp.dot(slopes[i, h, inner, :], q, preferred_element_type=F32) * factor
        terms[i, h, 1] = jnp.dot(probs[i, h, inner, :], go, preferred_element_type=F32)

    def h_copy(i, h, t):
        return remote(
            halo_send.at[i, h, t], halo_recv.at[i, h, t], sent_bwd if i == 0 else sent_fwd,
            h_recv.at[i, h, t], bwd_id if i == 0 else fwd_id,
        )

    results = (gq_ref, gk_ref, gv_ref)

    def out_copy(t, o, h):
        source = dq.at[h] if t == 0 else dkv.at[h, t - 1]
        return remote(
            source.at[slab(peers[o]), :], results[t].at[:, lanes(r, h)],
            sent, out_recv.at[t], peer_id(o),
        )

    def out_local(t, h):
        source = dq.at[h] if t == 0 else dkv.at[h, t - 1]
        return pltpu.make_async_copy(
            source.at[slab(r), :], results[t].at[:, lanes(r, h)], out_recv.at[t]
        )

    def sums(t, h):
        @pl.when(has_fwd)
        def _():
            with scope("wait_h0"):
                arrived(halo_recv.at[0, h, t], h_recv.at[0, h, t])

        @pl.when(has_bwd)
        def _():
            with scope("wait_h1"):
                arrived(halo_recv.at[1, h, t], h_recv.at[1, h, t])

        with scope("sums"):
            for i in range(2):
                half = pl.multiple_of(y * block if i == 0 else (1 - y) * block, block)
                out = pl.ds(half, block)
                total = terms[0, h, t, out, :] + terms[1, h, t, out, :]
                total = total + halo_recv[i, h, t].astype(F32)
                dkv[h, t, out, :] = total.astype(BF16)
        for o in (2, 3, 1):
            out_copy(1 + t, o, h).start()
        out_local(1 + t, h).start()

    def send_edge(t, i, h):
        with scope("edge"):
            (edge_keys, edge_values)[t](i, h)

        @pl.when(has_bwd if i == 0 else has_fwd)
        def _():
            h_copy(i, h, t).start()

    for h in range(heads):
        with scope("wait_go"):
            arrived(gos.at[h], go_recv.at[h])
        for i in range(2):
            send_edge(1, i, h)
        for i in range(2):
            send_edge(0, i, h)
            if h > 0:
                sums(1 - i, h - 1)
            with scope("query"):
                query_terms(i, h)
            if i == 0:
                out_copy(0, 2, h).start()
                out_copy(0, 3, h).start()
            else:
                out_copy(0, 1, h).start()
                out_local(0, h).start()
        with scope("inner"):
            for i in range(2):
                inner_terms(i, h)
    for t in (1, 0):
        sums(t, heads - 1)

    def mixed_copy(n):
        return pltpu.make_async_copy(
            mixed_out.at[n], mixed_ref.at[:, part(n)], mixed_sem
        )

    for n in range(chunks):
        with scope("wait_part"):
            p_copy(n).wait_recv()
        with scope("mixed"):
            total = part_own[n] + part_recv[n].astype(F32)
            mixed_out[n] = total.astype(BF16)
        mixed_copy(n).start()

    far_sends = (3 + 1 + 1 + 3) * (GROUP - 1) * rows * heads * width
    sent_rows = (far_sends + 2 * rows * feats) // feats
    arrived(w_own.at[pl.ds(0, sent_rows), :], sent)
    side_rows = (2 * 2 * rows + 2 * halo) * heads * width // feats

    @pl.when(has_fwd)
    def _():
        arrived(w_own.at[pl.ds(0, side_rows), :], sent_fwd)

    @pl.when(has_bwd)
    def _():
        arrived(w_own.at[pl.ds(0, side_rows), :], sent_bwd)

    with scope("end"):
        for t in range(3):
            arrived(results[t], out_recv.at[t])
        arrived(mixed_ref, mixed_sem)


def store_kernel(*refs):
    count = (len(refs) - 1) // 2
    copies = [
        pltpu.make_async_copy(refs[i], refs[count + i], refs[-1].at[i]) for i in range(count)
    ]
    for copy in copies:
        copy.start()
    for copy in copies:
        copy.wait()


def store(arrays):
    place = pl.BlockSpec(memory_space=pltpu.HBM)
    return pl.pallas_call(
        store_kernel,
        in_specs=[pl.BlockSpec(memory_space=pltpu.VMEM)] * len(arrays),
        out_specs=[place] * len(arrays),
        out_shape=[jax.ShapeDtypeStruct(a.shape, a.dtype) for a in arrays],
        scratch_shapes=[pltpu.SemaphoreType.DMA((len(arrays),))],
        compiler_params=pltpu.CompilerParams(vmem_limit_bytes=4 * 1024 * 1024),
    )(*arrays)


def fused(queries, keys, values, out_weight, mixed_grad, lengths, dilation, groups, chunks=4):
    rows, cols = queries.shape
    width = HEAD_WIDTH
    heads = cols // GROUP // width
    feats = mixed_grad.shape[1]
    step = feats // chunks
    block, halo, tokens = 2 * rows, 2 * rows, GROUP * rows
    window = block + 2 * halo
    hbm = pl.BlockSpec(memory_space=pltpu.HBM)
    vmem = pl.BlockSpec(memory_space=pl.ANY)
    dma = pltpu.SemaphoreType.DMA
    V = pltpu.VMEM
    one = jax.ShapeDtypeStruct((rows, cols), BF16)
    big = [
        pltpu.with_memory_space_constraint(a, pltpu.HBM)
        for a in (lengths, dilation, queries, keys, values, out_weight, mixed_grad)
    ]
    outs = pl.pallas_call(
        functools.partial(fused_kernel, groups),
        in_specs=[hbm] * 7,
        out_specs=[vmem] * 4,
        out_shape=[jax.ShapeDtypeStruct((rows, feats), BF16), one, one, one],
        scratch_shapes=[
            V((cols, feats), BF16), V((cols, feats), BF16),
            V((rows, feats), BF16), V((chunks, rows, step), BF16),
            V((heads, 2, tokens + 2 * halo, width), BF16),
            V((heads, tokens, width), BF16), V((heads, tokens, width), BF16),
            V((rows, cols), F32), V((rows, cols), BF16),
            V((heads, tokens, width), BF16), V((rows, cols), BF16),
            V((chunks, rows, step), BF16), V((chunks, rows, step), BF16), V((chunks, rows, step), F32),
            V((2, heads, window, block), BF16), V((heads, window, block), jnp.int32),
            V((2, heads, 8, block), jnp.int32), V((2, heads, 2, 2 * block, width), F32),
            V((2, heads, window, block), BF16),
            V((2, heads, 2, halo, width), BF16), V((2, heads, 2, halo, width), BF16),
            V((heads, tokens, width), BF16), V((heads, 2, tokens, width), BF16),
            V((chunks, rows, step), BF16), pltpu.SMEM(lengths.shape, jnp.int32), pltpu.SMEM(dilation.shape, jnp.int32),
            dma((2,)), dma((2,)), dma, dma, dma((chunks,)), dma((GROUP - 1, heads)), dma((heads,)),
            dma((2, heads)), dma((heads,)), dma, dma((chunks,)), dma((2, heads, 2)), dma((3,)), dma,
            dma, dma, dma,
        ],
        compiler_params=pltpu.CompilerParams(
            collective_id=0, has_side_effects=True, vmem_limit_bytes=32 * 1024 * 1024
        ),
    )(*big)
    return tuple(store(outs))


def attend_kernel(
    row_count, total, factor, first, index_ref, length_ref, dilation_ref,
    q_ref, go_ref, own_ref, a_ref, b_ref, po_ref, pa_ref,
    att_ref, gq_ref, own_t, a_t, b_t, po_t, pa_t, dist,
):
    slabs = (own_ref, a_ref, b_ref, po_ref, pa_ref)
    outs = (own_t, a_t, b_t, po_t, pa_t)

    @pl.when(pl.program_id(0) == 0)
    def _():
        me = index_ref[0]
        sign = 1 - 2 * lax.rem(me, 2)
        ends = [length_ref[0]]
        for n in range(1, length_ref.shape[0]):
            ends.append(ends[-1] + length_ref[n])

        def segment(pos):
            seg = jnp.zeros(pos.shape, jnp.int32)
            for end in ends:
                seg = seg + (pos >= end).astype(jnp.int32)
            return seg

        qpos = me * row_count + lax.broadcasted_iota(jnp.int32, (1, row_count), 1)
        qseg = segment(qpos)
        for i, off in enumerate((0, 2, -2, 1, -1)):
            kpos = (me + sign * off) * row_count + lax.broadcasted_iota(
                jnp.int32, (row_count, row_count), 0
            )
            same = (segment(kpos) == qseg) & (kpos >= 0) & (kpos < total)
            gap = jnp.abs(kpos - qpos).astype(jnp.float32)
            dist[pl.ds(i * row_count, row_count), :] = jnp.where(same, gap, FAR)

    spacing = jnp.full((1, row_count), dilation_ref[first + pl.program_id(0)], jnp.int32)
    inv = 1.0 / spacing.astype(jnp.float32)
    steps = dist[...] * inv
    whole = jnp.floor(steps + 0.5)
    mask = (whole <= HALF) & (jnp.abs(steps - whole) < 0.01)
    q = q_ref[...]
    go = go_ref[...]
    k = jnp.concatenate([r[0] for r in slabs], axis=0)
    v = jnp.concatenate([r[1] for r in slabs], axis=0)
    nt = (((1,), (1,)), ((), ()))
    tn = (((0,), (0,)), ((), ()))
    f32 = jnp.float32
    scores = lax.dot_general(k, q, nt, preferred_element_type=f32) * factor
    scores = jnp.where(mask, scores, NEG)
    top = jnp.max(scores, axis=0, keepdims=True)
    e = jnp.exp(scores - top)
    w = e * (1.0 / jnp.sum(e, axis=0, keepdims=True))
    p = w.astype(jnp.bfloat16)
    gp = lax.dot_general(v, go, nt, preferred_element_type=f32)
    delta = jnp.sum(w * gp, axis=0, keepdims=True)
    s = (w * (gp - delta)).astype(jnp.bfloat16)
    att_ref[...] = lax.dot_general(p, v, tn, preferred_element_type=f32).astype(jnp.bfloat16)
    gq_ref[...] = (
        lax.dot_general(s, k, tn, preferred_element_type=f32) * factor
    ).astype(jnp.bfloat16)
    kt = (jnp.dot(s, q, preferred_element_type=f32) * factor).astype(jnp.bfloat16)
    vt = jnp.dot(p, go, preferred_element_type=f32).astype(jnp.bfloat16)
    for i, out in enumerate(outs):
        out[0] = kt[i * row_count : (i + 1) * row_count]
        out[1] = vt[i * row_count : (i + 1) * row_count]


def attend(index, lengths, dilation, q, go, slabs, first, total, factor, width):
    rows, cols = q.shape[0], slabs[0].shape[2]
    heads = cols // width
    smem = pl.BlockSpec(memory_space=pltpu.SMEM)
    shared = pl.BlockSpec((rows, width), lambda h: (0, first + h))
    flat = pl.BlockSpec((rows, width), lambda h: (0, h))
    pair = pl.BlockSpec((2, rows, width), lambda h: (0, 0, h))
    one = jax.ShapeDtypeStruct((rows, cols), jnp.bfloat16)
    two = jax.ShapeDtypeStruct((2, rows, cols), jnp.bfloat16)
    return pl.pallas_call(
        functools.partial(attend_kernel, rows, total, factor, first),
        grid=(heads,),
        in_specs=[smem, smem, smem, shared, shared] + [pair] * 5,
        out_specs=[flat, flat] + [pair] * 5,
        out_shape=[one, one] + [two] * 5,
        scratch_shapes=[pltpu.VMEM((5 * rows, rows), jnp.float32)],
        compiler_params=pltpu.CompilerParams(dimension_semantics=("arbitrary",)),
        cost_estimate=pl.CostEstimate(
            flops=heads * 6 * 2 * 5 * rows * rows * width * 8,
            bytes_accessed=24 * 2 * rows * cols,
            transcendentals=heads * 5 * rows * rows,
        ),
    )(index, lengths, dilation, q, go, *slabs)


def per_device(queries, keys, values, out_weight, mixed_grad, lengths, dilation):
    rows = queries.shape[0]
    local_heads = dilation.shape[0]
    width = queries.shape[1] // local_heads
    factor = width ** (-0.5)
    count = lax.axis_size("ctx")
    sides = lax.axis_size("head")
    total = rows * count
    assert 2 * rows >= HALF * MAXD and count % 2 == 0
    if sides == 2 and count % GROUP == 0 and local_heads % GROUP == 0 and width == HEAD_WIDTH:
        if 2 * rows == HALF * MAXD and mixed_grad.shape[1] % 512 == 0:
            return fused(
                queries, keys, values, out_weight, mixed_grad, lengths, dilation, count // GROUP
            )
    index = lax.axis_index("ctx").astype(jnp.int32).reshape(1)

    inward = [
        (j, t) for j in range(count) for t in [j - 2 if j % 2 == 0 else j + 2] if 0 <= t < count
    ]
    outward = [(t, j) for j, t in inward]
    swapped = [(j, j ^ 1) for j in range(count)]

    def move(x, pairs):
        return lax.ppermute(x, "ctx", pairs)

    groups = 1
    gh = local_heads // groups
    cut = [slice(g * gh * width, (g + 1) * gh * width) for g in range(groups)]
    half = mixed_grad.shape[1]
    if sides == 2:
        other = lax.ppermute(mixed_grad, "head", [(0, 1), (1, 0)])
        left = lax.axis_index("head") == 0
        grad_full = jnp.concatenate(
            [jnp.where(left, mixed_grad, other), jnp.where(left, other, mixed_grad)], axis=1
        )
    else:
        grad_full = lax.all_gather(mixed_grad, "head", axis=1, tiled=True)
    stacks = []
    for g in range(groups):
        own = jnp.stack([keys[:, cut[g]], values[:, cut[g]]])
        stacks.append([own, move(own, inward), move(own, outward), move(own, swapped)])
    grad_attention = lax.dot_general(
        grad_full, out_weight, (((1,), (1,)), ((), ())), preferred_element_type=jnp.float32
    ).astype(jnp.bfloat16)

    atts, gqs, gkvs = [], [], []
    f32 = jnp.float32
    for slabs in stacks:
        slabs[1], grad_attention = lax.optimization_barrier((slabs[1], grad_attention))
        slabs.append(move(slabs[1], swapped))
    for g in range(groups):
        att, gq, own_t, a_t, b_t, po_t, pa_t = attend(
            index, lengths, dilation, queries, grad_attention, stacks[g], g * gh, total, factor, width
        )
        pa_back = move(pa_t, swapped)
        b_back = move(b_t, inward)
        po_back = move(po_t, swapped)
        a_sum = (a_t.astype(f32) + pa_back.astype(f32)).astype(jnp.bfloat16)
        a_sum, att = lax.optimization_barrier((a_sum, att))
        a_back = move(a_sum, outward)
        terms = (own_t, po_back, b_back, a_back)
        gkvs.append(
            [sum(term[i].astype(f32) for term in terms).astype(jnp.bfloat16) for i in range(2)]
        )
        atts.append(att)
        gqs.append(gq)
    attention = jnp.concatenate(atts, axis=1)
    partial = jnp.dot(attention, out_weight, preferred_element_type=f32)
    if sides == 2:
        lo, hi = partial[:, :half], partial[:, half:]
        away = jnp.where(left, hi, lo).astype(jnp.bfloat16)
        came = lax.ppermute(away, "head", [(0, 1), (1, 0)])
        mixed = (jnp.where(left, lo, hi) + came.astype(f32)).astype(jnp.bfloat16)
    else:
        mixed = lax.psum_scatter(
            partial.astype(jnp.bfloat16), "head", scatter_dimension=1, tiled=True
        )
    grad_keys, grad_values = (
        jnp.concatenate([pair[i] for pair in gkvs], axis=1) for i in range(2)
    )
    return mixed, jnp.concatenate(gqs, axis=1), grad_keys, grad_values


def solution(mesh):
    both = P("ctx", "head")
    return jax.shard_map(
        per_device,
        mesh=mesh,
        in_specs=(both, both, both, P("head", None), both, P(), P("head")),
        out_specs=(both, both, both, both),
        check_vma=False,
    )
```

```python
import functools
import jax
import jax.numpy as jnp
from jax import lax
from jax.experimental import pallas as pl
from jax.experimental.pallas import tpu as pltpu
from jax.sharding import PartitionSpec as P

HALF = 32
MAXD = 8
FAR = 1e6
NEG = -1e30
HEAD_WIDTH = 128

GROUP = 4
NT = (((1,), (1,)), ((), ()))
TN = (((0,), (0,)), ((), ()))
F32 = jnp.float32
LOG2E = 1.4426950408889634
BF16 = jnp.bfloat16
MESH_ID = pl.DeviceIdType.MESH


def fused_kernel(
    groups, length_hbm, dilation_hbm, q_ref, k_ref, v_ref, w_ref, mg_ref,
    mixed_ref, gq_ref, gk_ref, gv_ref,
    w_own, w_oth, mg_own, mg_oth, kv, qs, gos, go_acc, go_bf, att_my, att_in,
    part_send, part_recv, part_own, probs, spaced, bias, terms,
    slopes, halo_send, halo_recv, dq, dkv, mixed_out, length_ref, dilation_ref,
    int_sem, w_sem, mg_sem, own_sem, x_recv, kv_recv, q_recv, halo_kv, go_recv, att_recv,
    p_recv, h_recv, out_recv, mixed_sem, sent, sent_fwd, sent_bwd,
):
    rows = q_ref.shape[0]
    width = HEAD_WIDTH
    heads = q_ref.shape[1] // GROUP // width
    feats = mg_ref.shape[1]
    chunks = mg_oth.shape[0]
    step = feats // chunks
    window = kv.shape[2] - 2 * rows
    block = 2 * rows
    halo = 2 * rows
    factor = width ** (-0.5)
    scope = jax.named_scope

    c = lax.axis_index("ctx")
    side = lax.axis_index("head")
    g = c // GROUP
    r = c % GROUP
    y = r // 2
    core = r % 2
    peers = (r, r + 1 - 2 * core, r + 2 - 4 * y, (GROUP - 1) - r)
    base = g * GROUP
    ahead = 2 * y - 1
    has_fwd = (g + ahead >= 0) & (g + ahead < groups)
    has_bwd = (g - ahead >= 0) & (g - ahead < groups)
    fwd_id = {"ctx": c + GROUP * ahead}
    bwd_id = {"ctx": c - GROUP * ahead}
    x_id = {"head": 1 - side}

    def peer_id(o):
        return {"ctx": base + peers[o]}

    def lanes(i, h):
        return pl.ds(pl.multiple_of((i * heads + h) * width, width), width)

    def slab(i, first=0):
        return pl.ds(pl.multiple_of(first + i * rows, rows), rows)

    def arrived(ref, sem):
        pltpu.make_async_copy(ref, ref, sem).wait()

    def remote(src, dst, send, recv, device):
        return pltpu.make_async_remote_copy(
            src_ref=src, dst_ref=dst, send_sem=send, recv_sem=recv,
            device_id=device, device_id_type=MESH_ID,
        )

    integers = (
        pltpu.make_async_copy(length_hbm, length_ref, int_sem.at[0]),
        pltpu.make_async_copy(dilation_hbm, dilation_ref, int_sem.at[1]),
    )
    for copy in integers:
        copy.start()

    barrier = pltpu.get_barrier_semaphore()
    for o in (1, 2, 3):
        pl.semaphore_signal(barrier, inc=1, device_id=peer_id(o), device_id_type=MESH_ID)
    pl.semaphore_signal(barrier, inc=1, device_id=x_id, device_id_type=MESH_ID)

    @pl.when(has_fwd)
    def _():
        pl.semaphore_signal(barrier, inc=1, device_id=fwd_id, device_id_type=MESH_ID)

    @pl.when(has_bwd)
    def _():
        pl.semaphore_signal(barrier, inc=1, device_id=bwd_id, device_id_type=MESH_ID)

    def w_copy(half):
        where = side if half == 0 else 1 - side
        return pltpu.make_async_copy(
            w_ref.at[:, pl.ds(pl.multiple_of(where * feats, feats), feats)],
            (w_own, w_oth)[half], w_sem.at[half],
        )

    def part(n):
        return slice(n * step, (n + 1) * step)

    def in_place(t, h):
        return kv.at[h, t, slab(r, halo), :] if t < 2 else qs.at[h, slab(r), :]

    def own(t, h):
        source = (k_ref, v_ref, q_ref)[t].at[:, lanes(r, h)]
        return pltpu.make_async_copy(source, in_place(t, h), own_sem if t < 2 else q_recv.at[0, h])

    mg_copy = pltpu.make_async_copy(mg_ref, mg_own, mg_sem)
    for h in range(heads):
        own(0, h).start()
        own(1, h).start()
    mg_copy.start()
    w_copy(0).start()
    for h in range(heads):
        own(2, h).start()

    neighbours = has_fwd.astype(jnp.int32) + has_bwd.astype(jnp.int32)
    with scope("barrier"):
        pl.semaphore_wait(barrier, GROUP + neighbours)

    def x_copy(n):
        return remote(
            mg_ref.at[:, pl.ds(n * step, step)], mg_oth.at[n], sent, x_recv.at[n], x_id
        )

    def in_copy(t, o, h):
        source = (k_ref, v_ref, q_ref)[t].at[:, lanes(peers[o], h)]
        recv = kv_recv.at[o - 1, h] if t < 2 else q_recv.at[o // 2, h]
        return remote(source, in_place(t, h), sent, recv, peer_id(o))

    with scope("send"):
        x_copy(0).start()
        for h in range(heads):
            for t, o in ((0, 2), (1, 2), (0, 3), (1, 3), (0, 1), (1, 1)):
                in_copy(t, o, h).start()
        for n in range(1, chunks):
            x_copy(n).start()
        for h in range(heads):
            for o in (2, 3, 1):
                in_copy(2, o, h).start()
        w_copy(1).start()

    def relay(o, h):
        to = ahead if o < 2 else -ahead
        src_row = halo + peers[o] * rows
        dst_row = src_row - to * (GROUP * rows)
        return remote(
            kv.at[h, :, pl.ds(pl.multiple_of(src_row, rows), rows), :],
            kv.at[h, :, pl.ds(pl.multiple_of(dst_row, rows), rows), :],
            sent_fwd if o < 2 else sent_bwd, halo_kv.at[o // 2, h], fwd_id if o < 2 else bwd_id,
        )

    def pass_on(o, h):
        if o > 0:
            arrived(kv.at[h, :, slab(peers[o], halo), :], kv_recv.at[o - 1, h])

        @pl.when(has_fwd if o < 2 else has_bwd)
        def _():
            relay(o, h).start()

    near_row = pl.multiple_of((halo + GROUP * rows) * (1 - y), halo)
    far_row = pl.multiple_of((halo + GROUP * rows) * y, halo)

    @pl.when(jnp.logical_not(has_bwd))
    def _():
        for h in range(heads):
            kv[h, :, pl.ds(near_row, halo), :] = jnp.zeros((2, halo, width), BF16)
        halo_recv[1] = jnp.zeros(halo_recv.shape[1:], BF16)

    @pl.when(jnp.logical_not(has_fwd))
    def _():
        for h in range(heads):
            kv[h, :, pl.ds(far_row, halo), :] = jnp.zeros((2, halo, width), BF16)
        halo_recv[0] = jnp.zeros(halo_recv.shape[1:], BF16)

    arrived(kv.at[:, :, slab(r, halo), :], own_sem)
    for h in range(heads):
        pass_on(0, h)

    for copy in integers:
        copy.wait()
    def masks(i):
        first = base * rows + (1 - y if i == 0 else y) * block
        qpos = first + lax.broadcasted_iota(jnp.int32, (1, block), 1)
        start = jnp.zeros((1, block), jnp.int32)
        stop = jnp.full((1, block), 1 << 24, jnp.int32)
        end = jnp.int32(0)
        for n in range(length_ref.shape[0]):
            end = end + length_ref[n]
            past = qpos >= end
            start = jnp.where(past, jnp.maximum(start, end), start)
            stop = jnp.where(past, stop, jnp.minimum(stop, end))
        for h in range(heads):
            reach = jnp.full((1, block), HALF * dilation_ref[r * heads + h], jnp.int32)
            lo = jnp.maximum(start - qpos, -reach)
            hi = jnp.minimum(stop - 1 - qpos, reach)
            rel = spaced[h]
            bias[i, h] = jnp.where((rel >= lo) & (rel <= hi), 0.0, NEG)

    with scope("spaced"):
        rel = lax.broadcasted_iota(jnp.int32, (window, block), 0) - halo
        rel = rel - lax.broadcasted_iota(jnp.int32, (window, block), 1)
        relf = rel.astype(F32)
        for h in range(heads):
            spacing = jnp.full((1, block), dilation_ref[r * heads + h], jnp.int32)
            inv = 1.0 / spacing.astype(F32)
            steps = relf * inv
            near = jnp.floor(steps + 0.5)
            spaced[h] = jnp.where(jnp.abs(steps - near) < 0.01, rel, 1 << 24)

    def go_step(mg, weight, first):
        term = lax.dot_general(mg, weight, NT, preferred_element_type=F32)
        if first:
            go_acc[...] = term
        else:
            go_acc[...] += term

    mg_copy.wait()
    w_copy(0).wait()
    for n in range(chunks):
        with scope("go_own"):
            go_step(mg_own[:, part(n)], w_own[:, part(n)], n == 0)

    def go_far(n):
        if n == 0:
            w_copy(1).wait()
        with scope("wait_x"):
            x_copy(n).wait_recv()
        with scope("go_far"):
            go_step(mg_oth[n], w_oth[:, part(n)], False)

    with scope("masks"):
        for i in range(2):
            masks(i)
    with scope("wait_kv"):
        for h in range(heads):
            pass_on(1, h)
        for h in range(heads):
            for o in (2, 3):
                pass_on(o, h)

    def at_rows(i):
        return pl.multiple_of((1 - y) * block if i == 0 else y * block, block)

    def whole(i):
        return pl.ds(at_rows(i), block), pl.ds(0, block)

    def far_part(o):
        return slab(peers[o]), slab(peers[o] - 2 * (1 - y))

    def forward(i, h):
        row0 = at_rows(i)
        k = kv[h, 0, pl.ds(row0, window), :]
        v = kv[h, 1, pl.ds(row0, window), :]
        q_rows = pl.ds(row0, block)
        s = lax.dot_general(k, qs[h, q_rows, :], NT, preferred_element_type=F32)
        s = s + bias[i, h]
        top = jnp.max(s, axis=0, keepdims=True)
        e = jnp.exp2((s - top) * (factor * LOG2E))
        w = e * (1.0 / jnp.sum(e, axis=0, keepdims=True))
        p = w.astype(BF16)
        probs[i, h] = p
        att = lax.dot_general(p, v, TN, preferred_element_type=F32)
        att_my[h, q_rows, :] = att.astype(BF16)

    def att_copy(o, h):
        return remote(
            att_my.at[h, slab(peers[o]), :], att_in.at[:, lanes(r, h)],
            sent, att_recv, peer_id(o),
        )

    def att_local(h):
        return pltpu.make_async_copy(
            att_my.at[h, slab(r), :], att_in.at[:, lanes(r, h)], att_recv
        )

    def near_block(h):
        @pl.when(has_bwd)
        def _():
            with scope("wait_near"):
                arrived(kv.at[h, :, pl.ds(near_row, halo), :], halo_kv.at[0, h])

        with scope("wait_q"):
            arrived(qs.at[h, pl.ds(at_rows(0), block), :], q_recv.at[1, h])
        with scope("forward"):
            forward(0, h)
        for o in (2, 3):
            att_copy(o, h).start()

    def far_blocks():
        @pl.when(has_fwd)
        def _():
            with scope("wait_far"):
                for h in range(heads):
                    arrived(kv.at[h, :, pl.ds(far_row, halo), :], halo_kv.at[1, h])

        with scope("wait_q"):
            for h in range(heads):
                arrived(qs.at[h, pl.ds(at_rows(1), block), :], q_recv.at[0, h])
        with scope("forward"):
            for h in range(heads):
                forward(1, h)
        for h in range(heads):
            att_copy(1, h).start()
            att_local(h).start()

    go_far(0)
    for h in range(heads):
        near_block(h)
    go_far(1)
    far_blocks()
    for n in range(2, chunks - 1):
        go_far(n)

    def go_copy(o, h):
        return remote(
            go_bf.at[:, lanes(peers[o], h)], gos.at[h, slab(r), :],
            sent, go_recv.at[o // 2 * (o - 1), h], peer_id(o),
        )

    def go_local(h):
        return pltpu.make_async_copy(go_bf.at[:, lanes(r, h)], gos.at[h, slab(r), :], go_recv.at[0, h])

    with scope("wait_x"):
        x_copy(chunks - 1).wait_recv()
    for h in range(heads):
        with scope("go_last"):
            for i in range(GROUP):
                at = slice((i * heads + h) * width, (i * heads + h + 1) * width)
                term = lax.dot_general(
                    mg_oth[chunks - 1], w_oth[at, part(chunks - 1)], NT, preferred_element_type=F32
                )
                go_bf[:, at] = (go_acc[:, at] + term).astype(BF16)
        for o in (2, 3, 1):
            go_copy(o, h).start()
        go_local(h).start()

    with scope("wait_att"):
        arrived(att_in, att_recv)

    def p_copy(n):
        return remote(part_send.at[n], part_recv.at[n], sent, p_recv.at[n], x_id)

    def project(n):
        with scope("proj_far"):
            term = jnp.dot(att_in[...], w_oth[:, part(n)], preferred_element_type=F32)
            part_send[n] = term.astype(BF16)
        p_copy(n).start()

    project(0)

    def edge_rows(i):
        return pl.ds(pl.multiple_of(2 * at_rows(i), block), block)

    def edge_values(i, h):
        go = gos[h, pl.ds(at_rows(i), block), :]
        dv = jnp.dot(probs[i, h, edge_rows(i), :], go, preferred_element_type=F32)
        halo_send[i, h, 1] = dv.astype(BF16)

    def slope_terms(i, h, q_rows, cols):
        v = kv[h, 1, pl.ds(at_rows(i), window), :]
        gp = lax.dot_general(v, gos[h, q_rows, :], NT, preferred_element_type=F32)
        w = probs[i, h, :, cols].astype(F32)
        delta = jnp.sum(w * gp, axis=0, keepdims=True)
        slopes[i, h, :, cols] = (w * (gp - delta)).astype(BF16)

    def edge_keys(i, h):
        q = qs[h, pl.ds(at_rows(i), block), :]
        dk = jnp.dot(slopes[i, h, edge_rows(i), :], q, preferred_element_type=F32) * factor
        halo_send[i, h, 0] = dk.astype(BF16)

    def query_terms(i, h, q_rows, cols):
        k = kv[h, 0, pl.ds(at_rows(i), window), :]
        gq = lax.dot_general(slopes[i, h, :, cols], k, TN, preferred_element_type=F32) * factor
        dq[h, q_rows, :] = gq.astype(BF16)

    def inner_terms(i, h):
        row0 = at_rows(i)
        q = qs[h, pl.ds(row0, block), :]
        go = gos[h, pl.ds(row0, block), :]
        inner = pl.ds(pl.multiple_of(halo - row0, block), 2 * block)
        terms[i, h, 0] = jnp.dot(slopes[i, h, inner, :], q, preferred_element_type=F32) * factor
        terms[i, h, 1] = jnp.dot(probs[i, h, inner, :], go, preferred_element_type=F32)

    def h_copy(i, h, t):
        return remote(
            halo_send.at[i, h, t], halo_recv.at[i, h, t], sent_bwd if i == 0 else sent_fwd,
            h_recv.at[i, h, t], bwd_id if i == 0 else fwd_id,
        )

    results = (gq_ref, gk_ref, gv_ref)

    def out_copy(t, o, h):
        source = dq.at[h] if t == 0 else dkv.at[h, t - 1]
        return remote(
            source.at[slab(peers[o]), :], results[t].at[:, lanes(r, h)],
            sent, out_recv.at[t], peer_id(o),
        )

    def out_local(t, h):
        source = dq.at[h] if t == 0 else dkv.at[h, t - 1]
        return pltpu.make_async_copy(
            source.at[slab(r), :], results[t].at[:, lanes(r, h)], out_recv.at[t]
        )

    def sums(i, t, h):
        @pl.when(has_fwd if i == 0 else has_bwd)
        def _():
            with scope("wait_far_sum" if i else "wait_near_sum"):
                arrived(halo_recv.at[i, h, t], h_recv.at[i, h, t])

        with scope("sums"):
            half = pl.multiple_of(y * block if i == 0 else (1 - y) * block, block)
            out = pl.ds(half, block)
            total = terms[0, h, t, out, :] + terms[1, h, t, out, :]
            total = total + halo_recv[i, h, t].astype(F32)
            dkv[h, t, out, :] = total.astype(BF16)
        if i == 0:
            out_copy(1 + t, 1, h).start()
            out_local(1 + t, h).start()
        else:
            out_copy(1 + t, 2, h).start()
            out_copy(1 + t, 3, h).start()

    def send_edge(t, i, h):
        with scope("edge"):
            (edge_keys, edge_values)[t](i, h)

        @pl.when(has_bwd if i == 0 else has_fwd)
        def _():
            h_copy(i, h, t).start()

    def own_queries(h):
        with scope("wait_go"):
            arrived(gos.at[h, pl.ds(at_rows(1), block), :], go_recv.at[0, h])
        send_edge(1, 1, h)
        with scope("slopes"):
            slope_terms(1, h, *whole(1))
        send_edge(0, 1, h)

    def far_queries(h):
        for group in ((2,), (3,)) if h == 0 else ((2, 3),):
            with scope("wait_go"):
                for o in group:
                    arrived(gos.at[h, slab(peers[o]), :], go_recv.at[o - 1, h])
            with scope("slopes"):
                at = whole(0) if len(group) == 2 else far_part(group[0])
                slope_terms(0, h, *at)
                query_terms(0, h, *at)
            for o in group:
                out_copy(0, o, h).start()

    own_queries(0)
    project(1)
    for h in range(heads):
        far_queries(h)
        send_edge(0, 0, h)
        send_edge(1, 0, h)
        if h > 0:
            sums(1, 0, h - 1)
        with scope("inner"):
            for i in range(2):
                inner_terms(i, h)
        if h + 1 < heads:
            own_queries(h + 1)
        sums(1, 1, h)
        if h + 2 < chunks:
            project(h + 2)
    for n in range(heads + 2, chunks):
        project(n)
    sums(1, 0, heads - 1)
    for h in range(heads):
        with scope("query"):
            query_terms(1, h, *whole(1))
        out_copy(0, 1, h).start()
        out_local(0, h).start()
    for h in range(heads):
        for t in (1, 0):
            sums(0, t, h)
    with scope("proj_own"):
        for n in range(chunks):
            part_own[n] = jnp.dot(att_in[...], w_own[:, part(n)], preferred_element_type=F32)

    def mixed_copy(n):
        return pltpu.make_async_copy(
            mixed_out.at[n], mixed_ref.at[:, part(n)], mixed_sem
        )

    for n in range(chunks):
        with scope("wait_part"):
            p_copy(n).wait_recv()
        with scope("mixed"):
            total = part_own[n] + part_recv[n].astype(F32)
            mixed_out[n] = total.astype(BF16)
        mixed_copy(n).start()

    far_sends = (3 + 1 + 1 + 3) * (GROUP - 1) * rows * heads * width
    sent_rows = (far_sends + 2 * rows * feats) // feats
    arrived(w_own.at[pl.ds(0, sent_rows), :], sent)
    side_rows = (2 * 2 * rows + 2 * halo) * heads * width // feats

    @pl.when(has_fwd)
    def _():
        arrived(w_own.at[pl.ds(0, side_rows), :], sent_fwd)

    @pl.when(has_bwd)
    def _():
        arrived(w_own.at[pl.ds(0, side_rows), :], sent_bwd)

    with scope("end"):
        for t in range(3):
            arrived(results[t], out_recv.at[t])
        arrived(mixed_ref, mixed_sem)


def store_kernel(*refs):
    count = (len(refs) - 1) // 2
    copies = [
        pltpu.make_async_copy(refs[i], refs[count + i], refs[-1].at[i]) for i in range(count)
    ]
    for copy in copies:
        copy.start()
    for copy in copies:
        copy.wait()


def store(arrays):
    place = pl.BlockSpec(memory_space=pltpu.HBM)
    return pl.pallas_call(
        store_kernel,
        in_specs=[pl.BlockSpec(memory_space=pltpu.VMEM)] * len(arrays),
        out_specs=[place] * len(arrays),
        out_shape=[jax.ShapeDtypeStruct(a.shape, a.dtype) for a in arrays],
        scratch_shapes=[pltpu.SemaphoreType.DMA((len(arrays),))],
        compiler_params=pltpu.CompilerParams(vmem_limit_bytes=4 * 1024 * 1024),
    )(*arrays)


def fused(queries, keys, values, out_weight, mixed_grad, lengths, dilation, groups, chunks=4):
    rows, cols = queries.shape
    width = HEAD_WIDTH
    heads = cols // GROUP // width
    feats = mixed_grad.shape[1]
    step = feats // chunks
    block, halo, tokens = 2 * rows, 2 * rows, GROUP * rows
    window = block + 2 * halo
    hbm = pl.BlockSpec(memory_space=pltpu.HBM)
    vmem = pl.BlockSpec(memory_space=pl.ANY)
    dma = pltpu.SemaphoreType.DMA
    V = pltpu.VMEM
    one = jax.ShapeDtypeStruct((rows, cols), BF16)
    big = [
        pltpu.with_memory_space_constraint(a, pltpu.HBM)
        for a in (lengths, dilation, queries, keys, values, out_weight, mixed_grad)
    ]
    outs = pl.pallas_call(
        functools.partial(fused_kernel, groups),
        in_specs=[hbm] * 7,
        out_specs=[vmem] * 4,
        out_shape=[jax.ShapeDtypeStruct((rows, feats), BF16), one, one, one],
        scratch_shapes=[
            V((cols, feats), BF16), V((cols, feats), BF16),
            V((rows, feats), BF16), V((chunks, rows, step), BF16),
            V((heads, 2, tokens + 2 * halo, width), BF16),
            V((heads, tokens, width), BF16), V((heads, tokens, width), BF16),
            V((rows, cols), F32), V((rows, cols), BF16),
            V((heads, tokens, width), BF16), V((rows, cols), BF16),
            V((chunks, rows, step), BF16), V((chunks, rows, step), BF16), V((chunks, rows, step), F32),
            V((2, heads, window, block), BF16), V((heads, window, block), jnp.int32),
            V((2, heads, window, block), F32), V((2, heads, 2, 2 * block, width), F32),
            V((2, heads, window, block), BF16),
            V((2, heads, 2, halo, width), BF16), V((2, heads, 2, halo, width), BF16),
            V((heads, tokens, width), BF16), V((heads, 2, tokens, width), BF16),
            V((chunks, rows, step), BF16), pltpu.SMEM(lengths.shape, jnp.int32), pltpu.SMEM(dilation.shape, jnp.int32),
            dma((2,)), dma((2,)), dma, dma, dma((chunks,)), dma((GROUP - 1, heads)), dma((2, heads)),
            dma((2, heads)), dma((3, heads)), dma, dma((chunks,)), dma((2, heads, 2)), dma((3,)), dma,
            dma, dma, dma,
        ],
        compiler_params=pltpu.CompilerParams(
            collective_id=0, has_side_effects=True, vmem_limit_bytes=32 * 1024 * 1024
        ),
    )(*big)
    return tuple(store(outs))


def attend_kernel(
    row_count, total, factor, first, index_ref, length_ref, dilation_ref,
    q_ref, go_ref, own_ref, a_ref, b_ref, po_ref, pa_ref,
    att_ref, gq_ref, own_t, a_t, b_t, po_t, pa_t, dist,
):
    slabs = (own_ref, a_ref, b_ref, po_ref, pa_ref)
    outs = (own_t, a_t, b_t, po_t, pa_t)

    @pl.when(pl.program_id(0) == 0)
    def _():
        me = index_ref[0]
        sign = 1 - 2 * lax.rem(me, 2)
        ends = [length_ref[0]]
        for n in range(1, length_ref.shape[0]):
            ends.append(ends[-1] + length_ref[n])

        def segment(pos):
            seg = jnp.zeros(pos.shape, jnp.int32)
            for end in ends:
                seg = seg + (pos >= end).astype(jnp.int32)
            return seg

        qpos = me * row_count + lax.broadcasted_iota(jnp.int32, (1, row_count), 1)
        qseg = segment(qpos)
        for i, off in enumerate((0, 2, -2, 1, -1)):
            kpos = (me + sign * off) * row_count + lax.broadcasted_iota(
                jnp.int32, (row_count, row_count), 0
            )
            same = (segment(kpos) == qseg) & (kpos >= 0) & (kpos < total)
            gap = jnp.abs(kpos - qpos).astype(jnp.float32)
            dist[pl.ds(i * row_count, row_count), :] = jnp.where(same, gap, FAR)

    spacing = jnp.full((1, row_count), dilation_ref[first + pl.program_id(0)], jnp.int32)
    inv = 1.0 / spacing.astype(jnp.float32)
    steps = dist[...] * inv
    whole = jnp.floor(steps + 0.5)
    mask = (whole <= HALF) & (jnp.abs(steps - whole) < 0.01)
    q = q_ref[...]
    go = go_ref[...]
    k = jnp.concatenate([r[0] for r in slabs], axis=0)
    v = jnp.concatenate([r[1] for r in slabs], axis=0)
    nt = (((1,), (1,)), ((), ()))
    tn = (((0,), (0,)), ((), ()))
    f32 = jnp.float32
    scores = lax.dot_general(k, q, nt, preferred_element_type=f32) * factor
    scores = jnp.where(mask, scores, NEG)
    top = jnp.max(scores, axis=0, keepdims=True)
    e = jnp.exp(scores - top)
    w = e * (1.0 / jnp.sum(e, axis=0, keepdims=True))
    p = w.astype(jnp.bfloat16)
    gp = lax.dot_general(v, go, nt, preferred_element_type=f32)
    delta = jnp.sum(w * gp, axis=0, keepdims=True)
    s = (w * (gp - delta)).astype(jnp.bfloat16)
    att_ref[...] = lax.dot_general(p, v, tn, preferred_element_type=f32).astype(jnp.bfloat16)
    gq_ref[...] = (
        lax.dot_general(s, k, tn, preferred_element_type=f32) * factor
    ).astype(jnp.bfloat16)
    kt = (jnp.dot(s, q, preferred_element_type=f32) * factor).astype(jnp.bfloat16)
    vt = jnp.dot(p, go, preferred_element_type=f32).astype(jnp.bfloat16)
    for i, out in enumerate(outs):
        out[0] = kt[i * row_count : (i + 1) * row_count]
        out[1] = vt[i * row_count : (i + 1) * row_count]


def attend(index, lengths, dilation, q, go, slabs, first, total, factor, width):
    rows, cols = q.shape[0], slabs[0].shape[2]
    heads = cols // width
    smem = pl.BlockSpec(memory_space=pltpu.SMEM)
    shared = pl.BlockSpec((rows, width), lambda h: (0, first + h))
    flat = pl.BlockSpec((rows, width), lambda h: (0, h))
    pair = pl.BlockSpec((2, rows, width), lambda h: (0, 0, h))
    one = jax.ShapeDtypeStruct((rows, cols), jnp.bfloat16)
    two = jax.ShapeDtypeStruct((2, rows, cols), jnp.bfloat16)
    return pl.pallas_call(
        functools.partial(attend_kernel, rows, total, factor, first),
        grid=(heads,),
        in_specs=[smem, smem, smem, shared, shared] + [pair] * 5,
        out_specs=[flat, flat] + [pair] * 5,
        out_shape=[one, one] + [two] * 5,
        scratch_shapes=[pltpu.VMEM((5 * rows, rows), jnp.float32)],
        compiler_params=pltpu.CompilerParams(dimension_semantics=("arbitrary",)),
        cost_estimate=pl.CostEstimate(
            flops=heads * 6 * 2 * 5 * rows * rows * width * 8,
            bytes_accessed=24 * 2 * rows * cols,
            transcendentals=heads * 5 * rows * rows,
        ),
    )(index, lengths, dilation, q, go, *slabs)


def per_device(queries, keys, values, out_weight, mixed_grad, lengths, dilation):
    rows = queries.shape[0]
    local_heads = dilation.shape[0]
    width = queries.shape[1] // local_heads
    factor = width ** (-0.5)
    count = lax.axis_size("ctx")
    sides = lax.axis_size("head")
    total = rows * count
    assert 2 * rows >= HALF * MAXD and count % 2 == 0
    if sides == 2 and count % GROUP == 0 and local_heads % GROUP == 0 and width == HEAD_WIDTH:
        if 2 * rows == HALF * MAXD and mixed_grad.shape[1] % 512 == 0:
            return fused(
                queries, keys, values, out_weight, mixed_grad, lengths, dilation, count // GROUP
            )
    index = lax.axis_index("ctx").astype(jnp.int32).reshape(1)

    inward = [
        (j, t) for j in range(count) for t in [j - 2 if j % 2 == 0 else j + 2] if 0 <= t < count
    ]
    outward = [(t, j) for j, t in inward]
    swapped = [(j, j ^ 1) for j in range(count)]

    def move(x, pairs):
        return lax.ppermute(x, "ctx", pairs)

    groups = 1
    gh = local_heads // groups
    cut = [slice(g * gh * width, (g + 1) * gh * width) for g in range(groups)]
    half = mixed_grad.shape[1]
    if sides == 2:
        other = lax.ppermute(mixed_grad, "head", [(0, 1), (1, 0)])
        left = lax.axis_index("head") == 0
        grad_full = jnp.concatenate(
            [jnp.where(left, mixed_grad, other), jnp.where(left, other, mixed_grad)], axis=1
        )
    else:
        grad_full = lax.all_gather(mixed_grad, "head", axis=1, tiled=True)
    stacks = []
    for g in range(groups):
        own = jnp.stack([keys[:, cut[g]], values[:, cut[g]]])
        stacks.append([own, move(own, inward), move(own, outward), move(own, swapped)])
    grad_attention = lax.dot_general(
        grad_full, out_weight, (((1,), (1,)), ((), ())), preferred_element_type=jnp.float32
    ).astype(jnp.bfloat16)

    atts, gqs, gkvs = [], [], []
    f32 = jnp.float32
    for slabs in stacks:
        slabs[1], grad_attention = lax.optimization_barrier((slabs[1], grad_attention))
        slabs.append(move(slabs[1], swapped))
    for g in range(groups):
        att, gq, own_t, a_t, b_t, po_t, pa_t = attend(
            index, lengths, dilation, queries, grad_attention, stacks[g], g * gh, total, factor, width
        )
        pa_back = move(pa_t, swapped)
        b_back = move(b_t, inward)
        po_back = move(po_t, swapped)
        a_sum = (a_t.astype(f32) + pa_back.astype(f32)).astype(jnp.bfloat16)
        a_sum, att = lax.optimization_barrier((a_sum, att))
        a_back = move(a_sum, outward)
        terms = (own_t, po_back, b_back, a_back)
        gkvs.append(
            [sum(term[i].astype(f32) for term in terms).astype(jnp.bfloat16) for i in range(2)]
        )
        atts.append(att)
        gqs.append(gq)
    attention = jnp.concatenate(atts, axis=1)
    partial = jnp.dot(attention, out_weight, preferred_element_type=f32)
    if sides == 2:
        lo, hi = partial[:, :half], partial[:, half:]
        away = jnp.where(left, hi, lo).astype(jnp.bfloat16)
        came = lax.ppermute(away, "head", [(0, 1), (1, 0)])
        mixed = (jnp.where(left, lo, hi) + came.astype(f32)).astype(jnp.bfloat16)
    else:
        mixed = lax.psum_scatter(
            partial.astype(jnp.bfloat16), "head", scatter_dimension=1, tiled=True
        )
    grad_keys, grad_values = (
        jnp.concatenate([pair[i] for pair in gkvs], axis=1) for i in range(2)
    )
    return mixed, jnp.concatenate(gqs, axis=1), grad_keys, grad_values


def solution(mesh):
    both = P("ctx", "head")
    return jax.shard_map(
        per_device,
        mesh=mesh,
        in_specs=(both, both, both, P("head", None), both, P(), P("head")),
        out_specs=(both, both, both, both),
        check_vma=False,
    )
```

```python
import functools
import jax
import jax.numpy as jnp
from jax import lax
from jax.experimental import pallas as pl
from jax.experimental.pallas import tpu as pltpu
from jax.sharding import PartitionSpec as P

HALF = 32
MAXD = 8
FAR = 1e6
NEG = -1e30
HEAD_WIDTH = 128

GROUP = 4
NT = (((1,), (1,)), ((), ()))
TN = (((0,), (0,)), ((), ()))
F32 = jnp.float32
LOG2E = 1.4426950408889634
BF16 = jnp.bfloat16
MESH_ID = pl.DeviceIdType.MESH


def fused_kernel(
    groups, length_hbm, dilation_hbm, q_ref, k_ref, v_ref, w_ref, mg_ref,
    mixed_ref, gq_ref, gk_ref, gv_ref,
    w_own, w_oth, mg_own, mg_oth, kv, qs, gos, go_acc, go_bf, att_my, att_in,
    part_send, part_recv, part_own, probs, spaced, bias, terms,
    slopes, halo_send, halo_recv, dq, dkv, mixed_out, length_ref, dilation_ref,
    int_sem, w_sem, mg_sem, own_sem, x_recv, kv_recv, q_recv, halo_kv, go_recv, att_recv,
    p_recv, h_recv, out_recv, mixed_sem, sent, sent_fwd, sent_bwd,
):
    rows = q_ref.shape[0]
    width = HEAD_WIDTH
    heads = q_ref.shape[1] // GROUP // width
    feats = mg_ref.shape[1]
    chunks = mg_oth.shape[0]
    step = feats // chunks
    window = kv.shape[2] - 2 * rows
    block = 2 * rows
    halo = 2 * rows
    factor = width ** (-0.5)
    scope = jax.named_scope

    c = lax.axis_index("ctx")
    side = lax.axis_index("head")
    g = c // GROUP
    r = c % GROUP
    y = r // 2
    core = r % 2
    peers = (r, r + 1 - 2 * core, r + 2 - 4 * y, (GROUP - 1) - r)
    base = g * GROUP
    ahead = 2 * y - 1
    has_fwd = (g + ahead >= 0) & (g + ahead < groups)
    has_bwd = (g - ahead >= 0) & (g - ahead < groups)
    fwd_id = {"ctx": c + GROUP * ahead}
    bwd_id = {"ctx": c - GROUP * ahead}
    x_id = {"head": 1 - side}

    def peer_id(o):
        return {"ctx": base + peers[o]}

    def lanes(i, h):
        return pl.ds(pl.multiple_of((i * heads + h) * width, width), width)

    def slab(i, first=0):
        return pl.ds(pl.multiple_of(first + i * rows, rows), rows)

    def arrived(ref, sem):
        pltpu.make_async_copy(ref, ref, sem).wait()

    def remote(src, dst, send, recv, device):
        return pltpu.make_async_remote_copy(
            src_ref=src, dst_ref=dst, send_sem=send, recv_sem=recv,
            device_id=device, device_id_type=MESH_ID,
        )

    integers = (
        pltpu.make_async_copy(length_hbm, length_ref, int_sem.at[0]),
        pltpu.make_async_copy(dilation_hbm, dilation_ref, int_sem.at[1]),
    )
    for copy in integers:
        copy.start()

    barrier = pltpu.get_barrier_semaphore()
    for o in (1, 2, 3):
        pl.semaphore_signal(barrier, inc=1, device_id=peer_id(o), device_id_type=MESH_ID)
    pl.semaphore_signal(barrier, inc=1, device_id=x_id, device_id_type=MESH_ID)

    @pl.when(has_fwd)
    def _():
        pl.semaphore_signal(barrier, inc=1, device_id=fwd_id, device_id_type=MESH_ID)

    @pl.when(has_bwd)
    def _():
        pl.semaphore_signal(barrier, inc=1, device_id=bwd_id, device_id_type=MESH_ID)

    def w_copy(half):
        where = side if half == 0 else 1 - side
        return pltpu.make_async_copy(
            w_ref.at[:, pl.ds(pl.multiple_of(where * feats, feats), feats)],
            (w_own, w_oth)[half], w_sem.at[half],
        )

    def part(n):
        return slice(n * step, (n + 1) * step)

    def in_place(t, h):
        return kv.at[h, t, slab(r, halo), :] if t < 2 else qs.at[h, slab(r), :]

    def own(t, h):
        source = (k_ref, v_ref, q_ref)[t].at[:, lanes(r, h)]
        return pltpu.make_async_copy(source, in_place(t, h), own_sem if t < 2 else q_recv.at[0, h])

    mg_copy = pltpu.make_async_copy(mg_ref, mg_own, mg_sem)
    for h in range(heads):
        own(0, h).start()
        own(1, h).start()
    mg_copy.start()
    w_copy(0).start()
    for h in range(heads):
        own(2, h).start()

    neighbours = has_fwd.astype(jnp.int32) + has_bwd.astype(jnp.int32)
    with scope("barrier"):
        pl.semaphore_wait(barrier, GROUP + neighbours)

    def x_copy(n):
        return remote(
            mg_ref.at[:, pl.ds(n * step, step)], mg_oth.at[n], sent, x_recv.at[n], x_id
        )

    def in_copy(t, o, h):
        source = (k_ref, v_ref, q_ref)[t].at[:, lanes(peers[o], h)]
        recv = kv_recv.at[o - 1, h] if t < 2 else q_recv.at[o // 2 * (o - 1), h]
        return remote(source, in_place(t, h), sent, recv, peer_id(o))

    with scope("send"):
        x_copy(0).start()
        for h in range(heads):
            for t, o in ((0, 2), (1, 2), (0, 3), (1, 3), (0, 1), (1, 1)):
                in_copy(t, o, h).start()
        for n in range(1, chunks):
            x_copy(n).start()
        for h in range(heads):
            for o in (2, 3, 1):
                in_copy(2, o, h).start()
        w_copy(1).start()

    def relay(o, h):
        to = ahead if o < 2 else -ahead
        src_row = halo + peers[o] * rows
        dst_row = src_row - to * (GROUP * rows)
        return remote(
            kv.at[h, :, pl.ds(pl.multiple_of(src_row, rows), rows), :],
            kv.at[h, :, pl.ds(pl.multiple_of(dst_row, rows), rows), :],
            sent_fwd if o < 2 else sent_bwd, halo_kv.at[o // 2, h], fwd_id if o < 2 else bwd_id,
        )

    def pass_on(o, h):
        if o > 0:
            arrived(kv.at[h, :, slab(peers[o], halo), :], kv_recv.at[o - 1, h])

        @pl.when(has_fwd if o < 2 else has_bwd)
        def _():
            relay(o, h).start()

    near_row = pl.multiple_of((halo + GROUP * rows) * (1 - y), halo)
    far_row = pl.multiple_of((halo + GROUP * rows) * y, halo)

    @pl.when(jnp.logical_not(has_bwd))
    def _():
        for h in range(heads):
            kv[h, :, pl.ds(near_row, halo), :] = jnp.zeros((2, halo, width), BF16)
        halo_recv[1] = jnp.zeros(halo_recv.shape[1:], BF16)

    @pl.when(jnp.logical_not(has_fwd))
    def _():
        for h in range(heads):
            kv[h, :, pl.ds(far_row, halo), :] = jnp.zeros((2, halo, width), BF16)
        halo_recv[0] = jnp.zeros(halo_recv.shape[1:], BF16)

    arrived(kv.at[:, :, slab(r, halo), :], own_sem)
    for h in range(heads):
        pass_on(0, h)

    for copy in integers:
        copy.wait()
    def masks(i):
        first = base * rows + (1 - y if i == 0 else y) * block
        qpos = first + lax.broadcasted_iota(jnp.int32, (1, block), 1)
        start = jnp.zeros((1, block), jnp.int32)
        stop = jnp.full((1, block), 1 << 24, jnp.int32)
        end = jnp.int32(0)
        for n in range(length_ref.shape[0]):
            end = end + length_ref[n]
            past = qpos >= end
            start = jnp.where(past, jnp.maximum(start, end), start)
            stop = jnp.where(past, stop, jnp.minimum(stop, end))
        for h in range(heads):
            reach = jnp.full((1, block), HALF * dilation_ref[r * heads + h], jnp.int32)
            lo = jnp.maximum(start - qpos, -reach)
            hi = jnp.minimum(stop - 1 - qpos, reach)
            rel = spaced[h]
            bias[i, h] = jnp.where((rel >= lo) & (rel <= hi), 0.0, NEG)

    with scope("spaced"):
        rel = lax.broadcasted_iota(jnp.int32, (window, block), 0) - halo
        rel = rel - lax.broadcasted_iota(jnp.int32, (window, block), 1)
        relf = rel.astype(F32)
        for h in range(heads):
            spacing = jnp.full((1, block), dilation_ref[r * heads + h], jnp.int32)
            inv = 1.0 / spacing.astype(F32)
            steps = relf * inv
            near = jnp.floor(steps + 0.5)
            spaced[h] = jnp.where(jnp.abs(steps - near) < 0.01, rel, 1 << 24)

    def go_step(mg, weight, first):
        term = lax.dot_general(mg, weight, NT, preferred_element_type=F32)
        if first:
            go_acc[...] = term
        else:
            go_acc[...] += term

    mg_copy.wait()
    w_copy(0).wait()
    for n in range(chunks):
        with scope("go_own"):
            go_step(mg_own[:, part(n)], w_own[:, part(n)], n == 0)

    def go_far(n):
        if n == 0:
            w_copy(1).wait()
        with scope("wait_x"):
            x_copy(n).wait_recv()
        with scope("go_far"):
            go_step(mg_oth[n], w_oth[:, part(n)], False)

    with scope("masks"):
        for i in range(2):
            masks(i)
    with scope("wait_kv"):
        for h in range(heads):
            pass_on(1, h)
        for h in range(heads):
            for o in (2, 3):
                pass_on(o, h)

    def at_rows(i):
        return pl.multiple_of((1 - y) * block if i == 0 else y * block, block)

    def whole(i):
        return pl.ds(at_rows(i), block), pl.ds(0, block)

    def far_part(o):
        return slab(peers[o]), slab(peers[o] - 2 * (1 - y))

    def forward(i, h, q_rows, cols):
        row0 = at_rows(i)
        k = kv[h, 0, pl.ds(row0, window), :]
        v = kv[h, 1, pl.ds(row0, window), :]
        s = lax.dot_general(k, qs[h, q_rows, :], NT, preferred_element_type=F32)
        s = s + bias[i, h, :, cols]
        top = jnp.max(s, axis=0, keepdims=True)
        e = jnp.exp2((s - top) * (factor * LOG2E))
        w = e * (1.0 / jnp.sum(e, axis=0, keepdims=True))
        p = w.astype(BF16)
        probs[i, h, :, cols] = p
        att = lax.dot_general(p, v, TN, preferred_element_type=F32)
        att_my[h, q_rows, :] = att.astype(BF16)

    def att_copy(o, h):
        return remote(
            att_my.at[h, slab(peers[o]), :], att_in.at[:, lanes(r, h)],
            sent, att_recv, peer_id(o),
        )

    def att_local(h):
        return pltpu.make_async_copy(
            att_my.at[h, slab(r), :], att_in.at[:, lanes(r, h)], att_recv
        )

    def near_block(h):
        @pl.when(has_bwd)
        def _():
            with scope("wait_near"):
                arrived(kv.at[h, :, pl.ds(near_row, halo), :], halo_kv.at[0, h])

        for group in ((2,), (3,)) if h == 0 else ((2, 3),):
            with scope("wait_q"):
                for o in group:
                    arrived(qs.at[h, slab(peers[o]), :], q_recv.at[o - 1, h])
            with scope("forward"):
                forward(0, h, *(whole(0) if len(group) == 2 else far_part(group[0])))
            for o in group:
                att_copy(o, h).start()

    def far_blocks():
        @pl.when(has_fwd)
        def _():
            with scope("wait_far"):
                for h in range(heads):
                    arrived(kv.at[h, :, pl.ds(far_row, halo), :], halo_kv.at[1, h])

        with scope("wait_q"):
            for h in range(heads):
                arrived(qs.at[h, pl.ds(at_rows(1), block), :], q_recv.at[0, h])
        with scope("forward"):
            for h in range(heads):
                forward(1, h, *whole(1))
        for h in range(heads):
            att_copy(1, h).start()
            att_local(h).start()

    go_far(0)
    for h in range(heads):
        near_block(h)
    go_far(1)
    far_blocks()
    for n in range(2, chunks - 1):
        go_far(n)

    def go_copy(o, h):
        return remote(
            go_bf.at[:, lanes(peers[o], h)], gos.at[h, slab(r), :],
            sent, go_recv.at[o // 2 * (o - 1), h], peer_id(o),
        )

    def go_local(h):
        return pltpu.make_async_copy(go_bf.at[:, lanes(r, h)], gos.at[h, slab(r), :], go_recv.at[0, h])

    with scope("wait_x"):
        x_copy(chunks - 1).wait_recv()
    for h in range(heads):
        with scope("go_last"):
            for i in range(GROUP):
                at = slice((i * heads + h) * width, (i * heads + h + 1) * width)
                term = lax.dot_general(
                    mg_oth[chunks - 1], w_oth[at, part(chunks - 1)], NT, preferred_element_type=F32
                )
                go_bf[:, at] = (go_acc[:, at] + term).astype(BF16)
        for o in (2, 3, 1):
            go_copy(o, h).start()
        go_local(h).start()

    with scope("wait_att"):
        arrived(att_in, att_recv)

    def p_copy(n, cols):
        return remote(
            part_send.at[n, :, cols], part_recv.at[n, :, cols], sent, p_recv.at[n], x_id
        )

    def project(n, pieces=1):
        size = step // pieces
        for i in range(pieces):
            with scope("proj_far"):
                at = n * step + i * size
                term = jnp.dot(
                    att_in[...], w_oth[:, at : at + size], preferred_element_type=F32
                )
                part_send[n, :, i * size : (i + 1) * size] = term.astype(BF16)
            p_copy(n, pl.ds(i * size, size)).start()

    project(0, 4)

    def edge_rows(i):
        return pl.ds(pl.multiple_of(2 * at_rows(i), block), block)

    def edge_values(i, h):
        go = gos[h, pl.ds(at_rows(i), block), :]
        dv = jnp.dot(probs[i, h, edge_rows(i), :], go, preferred_element_type=F32)
        halo_send[i, h, 1] = dv.astype(BF16)

    def slope_terms(i, h, q_rows, cols):
        v = kv[h, 1, pl.ds(at_rows(i), window), :]
        gp = lax.dot_general(v, gos[h, q_rows, :], NT, preferred_element_type=F32)
        w = probs[i, h, :, cols].astype(F32)
        delta = jnp.sum(w * gp, axis=0, keepdims=True)
        slopes[i, h, :, cols] = (w * (gp - delta)).astype(BF16)

    def edge_keys(i, h):
        q = qs[h, pl.ds(at_rows(i), block), :]
        dk = jnp.dot(slopes[i, h, edge_rows(i), :], q, preferred_element_type=F32) * factor
        halo_send[i, h, 0] = dk.astype(BF16)

    def query_terms(i, h, q_rows, cols):
        k = kv[h, 0, pl.ds(at_rows(i), window), :]
        gq = lax.dot_general(slopes[i, h, :, cols], k, TN, preferred_element_type=F32) * factor
        dq[h, q_rows, :] = gq.astype(BF16)

    def inner_terms(i, h):
        row0 = at_rows(i)
        q = qs[h, pl.ds(row0, block), :]
        go = gos[h, pl.ds(row0, block), :]
        inner = pl.ds(pl.multiple_of(halo - row0, block), 2 * block)
        terms[i, h, 0] = jnp.dot(slopes[i, h, inner, :], q, preferred_element_type=F32) * factor
        terms[i, h, 1] = jnp.dot(probs[i, h, inner, :], go, preferred_element_type=F32)

    def h_copy(i, h, t):
        return remote(
            halo_send.at[i, h, t], halo_recv.at[i, h, t], sent_bwd if i == 0 else sent_fwd,
            h_recv.at[i, h, t], bwd_id if i == 0 else fwd_id,
        )

    results = (gq_ref, gk_ref, gv_ref)

    def out_copy(t, o, h):
        source = dq.at[h] if t == 0 else dkv.at[h, t - 1]
        return remote(
            source.at[slab(peers[o]), :], results[t].at[:, lanes(r, h)],
            sent, out_recv.at[t], peer_id(o),
        )

    def out_local(t, h):
        source = dq.at[h] if t == 0 else dkv.at[h, t - 1]
        return pltpu.make_async_copy(
            source.at[slab(r), :], results[t].at[:, lanes(r, h)], out_recv.at[t]
        )

    def sums(i, t, h):
        @pl.when(has_fwd if i == 0 else has_bwd)
        def _():
            with scope("wait_far_sum" if i else "wait_near_sum"):
                arrived(halo_recv.at[i, h, t], h_recv.at[i, h, t])

        with scope("sums"):
            half = pl.multiple_of(y * block if i == 0 else (1 - y) * block, block)
            out = pl.ds(half, block)
            total = terms[0, h, t, out, :] + terms[1, h, t, out, :]
            total = total + halo_recv[i, h, t].astype(F32)
            dkv[h, t, out, :] = total.astype(BF16)
        if i == 0:
            out_copy(1 + t, 1, h).start()
            out_local(1 + t, h).start()
        else:
            out_copy(1 + t, 2, h).start()
            out_copy(1 + t, 3, h).start()

    def send_edge(t, i, h):
        with scope("edge"):
            (edge_keys, edge_values)[t](i, h)

        @pl.when(has_bwd if i == 0 else has_fwd)
        def _():
            h_copy(i, h, t).start()

    def own_queries(h):
        with scope("wait_go"):
            arrived(gos.at[h, pl.ds(at_rows(1), block), :], go_recv.at[0, h])
        send_edge(1, 1, h)
        with scope("slopes"):
            slope_terms(1, h, *whole(1))
        send_edge(0, 1, h)

    def far_queries(h):
        for group in ((2,), (3,)) if h == 0 else ((2, 3),):
            with scope("wait_go"):
                for o in group:
                    arrived(gos.at[h, slab(peers[o]), :], go_recv.at[o - 1, h])
            with scope("slopes"):
                at = whole(0) if len(group) == 2 else far_part(group[0])
                slope_terms(0, h, *at)
                query_terms(0, h, *at)
            for o in group:
                out_copy(0, o, h).start()

    own_queries(0)
    project(1)
    for h in range(heads):
        far_queries(h)
        send_edge(0, 0, h)
        send_edge(1, 0, h)
        if h > 0:
            sums(1, 0, h - 1)
        with scope("inner"):
            for i in range(2):
                inner_terms(i, h)
        if h + 1 < heads:
            own_queries(h + 1)
        sums(1, 1, h)
        if h + 2 < chunks:
            project(h + 2)
    for n in range(heads + 2, chunks):
        project(n)
    sums(1, 0, heads - 1)
    for h in range(heads):
        with scope("query"):
            query_terms(1, h, *whole(1))
        out_copy(0, 1, h).start()
        out_local(0, h).start()
    for h in range(heads):
        for t in (1, 0):
            sums(0, t, h)
    with scope("proj_own"):
        for n in range(chunks):
            part_own[n] = jnp.dot(att_in[...], w_own[:, part(n)], preferred_element_type=F32)

    def mixed_copy(n):
        return pltpu.make_async_copy(
            mixed_out.at[n], mixed_ref.at[:, part(n)], mixed_sem
        )

    for n in range(chunks):
        with scope("wait_part"):
            arrived(part_recv.at[n], p_recv.at[n])
        with scope("mixed"):
            total = part_own[n] + part_recv[n].astype(F32)
            mixed_out[n] = total.astype(BF16)
        mixed_copy(n).start()

    far_sends = (3 + 1 + 1 + 3) * (GROUP - 1) * rows * heads * width
    sent_rows = (far_sends + 2 * rows * feats) // feats
    arrived(w_own.at[pl.ds(0, sent_rows), :], sent)
    side_rows = (2 * 2 * rows + 2 * halo) * heads * width // feats

    @pl.when(has_fwd)
    def _():
        arrived(w_own.at[pl.ds(0, side_rows), :], sent_fwd)

    @pl.when(has_bwd)
    def _():
        arrived(w_own.at[pl.ds(0, side_rows), :], sent_bwd)

    with scope("end"):
        for t in range(3):
            arrived(results[t], out_recv.at[t])
        arrived(mixed_ref, mixed_sem)


def store_kernel(*refs):
    count = (len(refs) - 1) // 2
    copies = [
        pltpu.make_async_copy(refs[i], refs[count + i], refs[-1].at[i]) for i in range(count)
    ]
    for copy in copies:
        copy.start()
    for copy in copies:
        copy.wait()


def store(arrays):
    place = pl.BlockSpec(memory_space=pltpu.HBM)
    return pl.pallas_call(
        store_kernel,
        in_specs=[pl.BlockSpec(memory_space=pltpu.VMEM)] * len(arrays),
        out_specs=[place] * len(arrays),
        out_shape=[jax.ShapeDtypeStruct(a.shape, a.dtype) for a in arrays],
        scratch_shapes=[pltpu.SemaphoreType.DMA((len(arrays),))],
        compiler_params=pltpu.CompilerParams(vmem_limit_bytes=4 * 1024 * 1024),
    )(*arrays)


def fused(queries, keys, values, out_weight, mixed_grad, lengths, dilation, groups, chunks=4):
    rows, cols = queries.shape
    width = HEAD_WIDTH
    heads = cols // GROUP // width
    feats = mixed_grad.shape[1]
    step = feats // chunks
    block, halo, tokens = 2 * rows, 2 * rows, GROUP * rows
    window = block + 2 * halo
    hbm = pl.BlockSpec(memory_space=pltpu.HBM)
    vmem = pl.BlockSpec(memory_space=pl.ANY)
    dma = pltpu.SemaphoreType.DMA
    V = pltpu.VMEM
    one = jax.ShapeDtypeStruct((rows, cols), BF16)
    big = [
        pltpu.with_memory_space_constraint(a, pltpu.HBM)
        for a in (lengths, dilation, queries, keys, values, out_weight, mixed_grad)
    ]
    outs = pl.pallas_call(
        functools.partial(fused_kernel, groups),
        in_specs=[hbm] * 7,
        out_specs=[vmem] * 4,
        out_shape=[jax.ShapeDtypeStruct((rows, feats), BF16), one, one, one],
        scratch_shapes=[
            V((cols, feats), BF16), V((cols, feats), BF16),
            V((rows, feats), BF16), V((chunks, rows, step), BF16),
            V((heads, 2, tokens + 2 * halo, width), BF16),
            V((heads, tokens, width), BF16), V((heads, tokens, width), BF16),
            V((rows, cols), F32), V((rows, cols), BF16),
            V((heads, tokens, width), BF16), V((rows, cols), BF16),
            V((chunks, rows, step), BF16), V((chunks, rows, step), BF16), V((chunks, rows, step), F32),
            V((2, heads, window, block), BF16), V((heads, window, block), jnp.int32),
            V((2, heads, window, block), F32), V((2, heads, 2, 2 * block, width), F32),
            V((2, heads, window, block), BF16),
            V((2, heads, 2, halo, width), BF16), V((2, heads, 2, halo, width), BF16),
            V((heads, tokens, width), BF16), V((heads, 2, tokens, width), BF16),
            V((chunks, rows, step), BF16), pltpu.SMEM(lengths.shape, jnp.int32), pltpu.SMEM(dilation.shape, jnp.int32),
            dma((2,)), dma((2,)), dma, dma, dma((chunks,)), dma((GROUP - 1, heads)), dma((3, heads)),
            dma((2, heads)), dma((3, heads)), dma, dma((chunks,)), dma((2, heads, 2)), dma((3,)), dma,
            dma, dma, dma,
        ],
        compiler_params=pltpu.CompilerParams(
            collective_id=0, has_side_effects=True, vmem_limit_bytes=32 * 1024 * 1024
        ),
    )(*big)
    return tuple(store(outs))


def attend_kernel(
    row_count, total, factor, first, index_ref, length_ref, dilation_ref,
    q_ref, go_ref, own_ref, a_ref, b_ref, po_ref, pa_ref,
    att_ref, gq_ref, own_t, a_t, b_t, po_t, pa_t, dist,
):
    slabs = (own_ref, a_ref, b_ref, po_ref, pa_ref)
    outs = (own_t, a_t, b_t, po_t, pa_t)

    @pl.when(pl.program_id(0) == 0)
    def _():
        me = index_ref[0]
        sign = 1 - 2 * lax.rem(me, 2)
        ends = [length_ref[0]]
        for n in range(1, length_ref.shape[0]):
            ends.append(ends[-1] + length_ref[n])

        def segment(pos):
            seg = jnp.zeros(pos.shape, jnp.int32)
            for end in ends:
                seg = seg + (pos >= end).astype(jnp.int32)
            return seg

        qpos = me * row_count + lax.broadcasted_iota(jnp.int32, (1, row_count), 1)
        qseg = segment(qpos)
        for i, off in enumerate((0, 2, -2, 1, -1)):
            kpos = (me + sign * off) * row_count + lax.broadcasted_iota(
                jnp.int32, (row_count, row_count), 0
            )
            same = (segment(kpos) == qseg) & (kpos >= 0) & (kpos < total)
            gap = jnp.abs(kpos - qpos).astype(jnp.float32)
            dist[pl.ds(i * row_count, row_count), :] = jnp.where(same, gap, FAR)

    spacing = jnp.full((1, row_count), dilation_ref[first + pl.program_id(0)], jnp.int32)
    inv = 1.0 / spacing.astype(jnp.float32)
    steps = dist[...] * inv
    whole = jnp.floor(steps + 0.5)
    mask = (whole <= HALF) & (jnp.abs(steps - whole) < 0.01)
    q = q_ref[...]
    go = go_ref[...]
    k = jnp.concatenate([r[0] for r in slabs], axis=0)
    v = jnp.concatenate([r[1] for r in slabs], axis=0)
    nt = (((1,), (1,)), ((), ()))
    tn = (((0,), (0,)), ((), ()))
    f32 = jnp.float32
    scores = lax.dot_general(k, q, nt, preferred_element_type=f32) * factor
    scores = jnp.where(mask, scores, NEG)
    top = jnp.max(scores, axis=0, keepdims=True)
    e = jnp.exp(scores - top)
    w = e * (1.0 / jnp.sum(e, axis=0, keepdims=True))
    p = w.astype(jnp.bfloat16)
    gp = lax.dot_general(v, go, nt, preferred_element_type=f32)
    delta = jnp.sum(w * gp, axis=0, keepdims=True)
    s = (w * (gp - delta)).astype(jnp.bfloat16)
    att_ref[...] = lax.dot_general(p, v, tn, preferred_element_type=f32).astype(jnp.bfloat16)
    gq_ref[...] = (
        lax.dot_general(s, k, tn, preferred_element_type=f32) * factor
    ).astype(jnp.bfloat16)
    kt = (jnp.dot(s, q, preferred_element_type=f32) * factor).astype(jnp.bfloat16)
    vt = jnp.dot(p, go, preferred_element_type=f32).astype(jnp.bfloat16)
    for i, out in enumerate(outs):
        out[0] = kt[i * row_count : (i + 1) * row_count]
        out[1] = vt[i * row_count : (i + 1) * row_count]


def attend(index, lengths, dilation, q, go, slabs, first, total, factor, width):
    rows, cols = q.shape[0], slabs[0].shape[2]
    heads = cols // width
    smem = pl.BlockSpec(memory_space=pltpu.SMEM)
    shared = pl.BlockSpec((rows, width), lambda h: (0, first + h))
    flat = pl.BlockSpec((rows, width), lambda h: (0, h))
    pair = pl.BlockSpec((2, rows, width), lambda h: (0, 0, h))
    one = jax.ShapeDtypeStruct((rows, cols), jnp.bfloat16)
    two = jax.ShapeDtypeStruct((2, rows, cols), jnp.bfloat16)
    return pl.pallas_call(
        functools.partial(attend_kernel, rows, total, factor, first),
        grid=(heads,),
        in_specs=[smem, smem, smem, shared, shared] + [pair] * 5,
        out_specs=[flat, flat] + [pair] * 5,
        out_shape=[one, one] + [two] * 5,
        scratch_shapes=[pltpu.VMEM((5 * rows, rows), jnp.float32)],
        compiler_params=pltpu.CompilerParams(dimension_semantics=("arbitrary",)),
        cost_estimate=pl.CostEstimate(
            flops=heads * 6 * 2 * 5 * rows * rows * width * 8,
            bytes_accessed=24 * 2 * rows * cols,
            transcendentals=heads * 5 * rows * rows,
        ),
    )(index, lengths, dilation, q, go, *slabs)


def per_device(queries, keys, values, out_weight, mixed_grad, lengths, dilation):
    rows = queries.shape[0]
    local_heads = dilation.shape[0]
    width = queries.shape[1] // local_heads
    factor = width ** (-0.5)
    count = lax.axis_size("ctx")
    sides = lax.axis_size("head")
    total = rows * count
    assert 2 * rows >= HALF * MAXD and count % 2 == 0
    if sides == 2 and count % GROUP == 0 and local_heads % GROUP == 0 and width == HEAD_WIDTH:
        if 2 * rows == HALF * MAXD and mixed_grad.shape[1] % 512 == 0:
            return fused(
                queries, keys, values, out_weight, mixed_grad, lengths, dilation, count // GROUP
            )
    index = lax.axis_index("ctx").astype(jnp.int32).reshape(1)

    inward = [
        (j, t) for j in range(count) for t in [j - 2 if j % 2 == 0 else j + 2] if 0 <= t < count
    ]
    outward = [(t, j) for j, t in inward]
    swapped = [(j, j ^ 1) for j in range(count)]

    def move(x, pairs):
        return lax.ppermute(x, "ctx", pairs)

    groups = 1
    gh = local_heads // groups
    cut = [slice(g * gh * width, (g + 1) * gh * width) for g in range(groups)]
    half = mixed_grad.shape[1]
    if sides == 2:
        other = lax.ppermute(mixed_grad, "head", [(0, 1), (1, 0)])
        left = lax.axis_index("head") == 0
        grad_full = jnp.concatenate(
            [jnp.where(left, mixed_grad, other), jnp.where(left, other, mixed_grad)], axis=1
        )
    else:
        grad_full = lax.all_gather(mixed_grad, "head", axis=1, tiled=True)
    stacks = []
    for g in range(groups):
        own = jnp.stack([keys[:, cut[g]], values[:, cut[g]]])
        stacks.append([own, move(own, inward), move(own, outward), move(own, swapped)])
    grad_attention = lax.dot_general(
        grad_full, out_weight, (((1,), (1,)), ((), ())), preferred_element_type=jnp.float32
    ).astype(jnp.bfloat16)

    atts, gqs, gkvs = [], [], []
    f32 = jnp.float32
    for slabs in stacks:
        slabs[1], grad_attention = lax.optimization_barrier((slabs[1], grad_attention))
        slabs.append(move(slabs[1], swapped))
    for g in range(groups):
        att, gq, own_t, a_t, b_t, po_t, pa_t = attend(
            index, lengths, dilation, queries, grad_attention, stacks[g], g * gh, total, factor, width
        )
        pa_back = move(pa_t, swapped)
        b_back = move(b_t, inward)
        po_back = move(po_t, swapped)
        a_sum = (a_t.astype(f32) + pa_back.astype(f32)).astype(jnp.bfloat16)
        a_sum, att = lax.optimization_barrier((a_sum, att))
        a_back = move(a_sum, outward)
        terms = (own_t, po_back, b_back, a_back)
        gkvs.append(
            [sum(term[i].astype(f32) for term in terms).astype(jnp.bfloat16) for i in range(2)]
        )
        atts.append(att)
        gqs.append(gq)
    attention = jnp.concatenate(atts, axis=1)
    partial = jnp.dot(attention, out_weight, preferred_element_type=f32)
    if sides == 2:
        lo, hi = partial[:, :half], partial[:, half:]
        away = jnp.where(left, hi, lo).astype(jnp.bfloat16)
        came = lax.ppermute(away, "head", [(0, 1), (1, 0)])
        mixed = (jnp.where(left, lo, hi) + came.astype(f32)).astype(jnp.bfloat16)
    else:
        mixed = lax.psum_scatter(
            partial.astype(jnp.bfloat16), "head", scatter_dimension=1, tiled=True
        )
    grad_keys, grad_values = (
        jnp.concatenate([pair[i] for pair in gkvs], axis=1) for i in range(2)
    )
    return mixed, jnp.concatenate(gqs, axis=1), grad_keys, grad_values


def solution(mesh):
    both = P("ctx", "head")
    return jax.shard_map(
        per_device,
        mesh=mesh,
        in_specs=(both, both, both, P("head", None), both, P(), P("head")),
        out_specs=(both, both, both, both),
        check_vma=False,
    )
```

```python
import functools
import jax
import jax.numpy as jnp
from jax import lax
from jax.experimental import pallas as pl
from jax.experimental.pallas import tpu as pltpu
from jax.sharding import PartitionSpec as P

HALF = 32
MAXD = 8
FAR = 1e6
NEG = -1e30
HEAD_WIDTH = 128

GROUP = 4
NT = (((1,), (1,)), ((), ()))
TN = (((0,), (0,)), ((), ()))
F32 = jnp.float32
LOG2E = 1.4426950408889634
BF16 = jnp.bfloat16
MESH_ID = pl.DeviceIdType.MESH


def fused_kernel(
    groups, length_hbm, dilation_hbm, q_ref, k_ref, v_ref, w_ref, mg_ref,
    mixed_ref, gq_ref, gk_ref, gv_ref,
    w_own, w_oth, mg_own, mg_oth, kv, qs, gos, go_acc, go_bf, att_my, att_in,
    part_send, part_recv, part_own, probs, spaced, bias, terms,
    slopes, halo_send, halo_recv, dq, dkv, mixed_out, length_ref, dilation_ref,
    int_sem, w_sem, mg_sem, own_sem, x_recv, kv_recv, q_recv, halo_kv, go_recv, att_recv,
    p_recv, h_recv, out_recv, mixed_sem, sent, sent_fwd, sent_bwd,
):
    rows = q_ref.shape[0]
    width = HEAD_WIDTH
    heads = q_ref.shape[1] // GROUP // width
    feats = mg_ref.shape[1]
    chunks = mg_oth.shape[0]
    step = feats // chunks
    window = kv.shape[2] - 2 * rows
    block = 2 * rows
    halo = 2 * rows
    factor = width ** (-0.5)
    scope = jax.named_scope

    c = lax.axis_index("ctx")
    side = lax.axis_index("head")
    g = c // GROUP
    r = c % GROUP
    y = r // 2
    core = r % 2
    peers = (r, r + 1 - 2 * core, r + 2 - 4 * y, (GROUP - 1) - r)
    base = g * GROUP
    ahead = 2 * y - 1
    has_fwd = (g + ahead >= 0) & (g + ahead < groups)
    has_bwd = (g - ahead >= 0) & (g - ahead < groups)
    fwd_id = {"ctx": c + GROUP * ahead}
    bwd_id = {"ctx": c - GROUP * ahead}
    x_id = {"head": 1 - side}

    def peer_id(o):
        return {"ctx": base + peers[o]}

    def lanes(i, h):
        return pl.ds(pl.multiple_of((i * heads + h) * width, width), width)

    def slab(i, first=0):
        return pl.ds(pl.multiple_of(first + i * rows, rows), rows)

    def arrived(ref, sem):
        pltpu.make_async_copy(ref, ref, sem).wait()

    def remote(src, dst, send, recv, device):
        return pltpu.make_async_remote_copy(
            src_ref=src, dst_ref=dst, send_sem=send, recv_sem=recv,
            device_id=device, device_id_type=MESH_ID,
        )

    integers = (
        pltpu.make_async_copy(length_hbm, length_ref, int_sem.at[0]),
        pltpu.make_async_copy(dilation_hbm, dilation_ref, int_sem.at[1]),
    )
    for copy in integers:
        copy.start()

    barrier = pltpu.get_barrier_semaphore()
    for o in (1, 2, 3):
        pl.semaphore_signal(barrier, inc=1, device_id=peer_id(o), device_id_type=MESH_ID)
    pl.semaphore_signal(barrier, inc=1, device_id=x_id, device_id_type=MESH_ID)

    @pl.when(has_fwd)
    def _():
        pl.semaphore_signal(barrier, inc=1, device_id=fwd_id, device_id_type=MESH_ID)

    @pl.when(has_bwd)
    def _():
        pl.semaphore_signal(barrier, inc=1, device_id=bwd_id, device_id_type=MESH_ID)

    def w_copy(half):
        where = side if half == 0 else 1 - side
        return pltpu.make_async_copy(
            w_ref.at[:, pl.ds(pl.multiple_of(where * feats, feats), feats)],
            (w_own, w_oth)[half], w_sem.at[half],
        )

    def part(n):
        return slice(n * step, (n + 1) * step)

    def in_place(t, h):
        return kv.at[h, t, slab(r, halo), :] if t < 2 else qs.at[h, slab(r), :]

    def own(t, h):
        source = (k_ref, v_ref, q_ref)[t].at[:, lanes(r, h)]
        return pltpu.make_async_copy(source, in_place(t, h), own_sem if t < 2 else q_recv.at[0, h])

    mg_copy = pltpu.make_async_copy(mg_ref, mg_own, mg_sem)
    for h in range(heads):
        own(0, h).start()
        own(1, h).start()
    mg_copy.start()
    w_copy(0).start()
    for h in range(heads):
        own(2, h).start()

    neighbours = has_fwd.astype(jnp.int32) + has_bwd.astype(jnp.int32)
    with scope("barrier"):
        pl.semaphore_wait(barrier, GROUP + neighbours)

    def x_copy(n):
        return remote(
            mg_ref.at[:, pl.ds(n * step, step)], mg_oth.at[n], sent, x_recv.at[n], x_id
        )

    def in_copy(t, o, h):
        source = (k_ref, v_ref, q_ref)[t].at[:, lanes(peers[o], h)]
        recv = kv_recv.at[o - 1, h] if t < 2 else q_recv.at[o // 2 * (o - 1), h]
        return remote(source, in_place(t, h), sent, recv, peer_id(o))

    with scope("send"):
        x_copy(0).start()
        for h in range(heads):
            for t, o in ((0, 2), (1, 2), (0, 3), (1, 3), (0, 1), (1, 1)):
                in_copy(t, o, h).start()
        for n in range(1, chunks):
            x_copy(n).start()
        for h in range(heads):
            for o in (2, 3, 1):
                in_copy(2, o, h).start()
        w_copy(1).start()

    def relay(o, h):
        to = ahead if o < 2 else -ahead
        src_row = halo + peers[o] * rows
        dst_row = src_row - to * (GROUP * rows)
        return remote(
            kv.at[h, :, pl.ds(pl.multiple_of(src_row, rows), rows), :],
            kv.at[h, :, pl.ds(pl.multiple_of(dst_row, rows), rows), :],
            sent_fwd if o < 2 else sent_bwd, halo_kv.at[o // 2, h], fwd_id if o < 2 else bwd_id,
        )

    def pass_on(o, h):
        if o > 0:
            arrived(kv.at[h, :, slab(peers[o], halo), :], kv_recv.at[o - 1, h])

        @pl.when(has_fwd if o < 2 else has_bwd)
        def _():
            relay(o, h).start()

    near_row = pl.multiple_of((halo + GROUP * rows) * (1 - y), halo)
    far_row = pl.multiple_of((halo + GROUP * rows) * y, halo)

    @pl.when(jnp.logical_not(has_bwd))
    def _():
        for h in range(heads):
            kv[h, :, pl.ds(near_row, halo), :] = jnp.zeros((2, halo, width), BF16)
        halo_recv[1] = jnp.zeros(halo_recv.shape[1:], BF16)

    @pl.when(jnp.logical_not(has_fwd))
    def _():
        for h in range(heads):
            kv[h, :, pl.ds(far_row, halo), :] = jnp.zeros((2, halo, width), BF16)
        halo_recv[0] = jnp.zeros(halo_recv.shape[1:], BF16)

    arrived(kv.at[:, :, slab(r, halo), :], own_sem)
    for h in range(heads):
        pass_on(0, h)

    for copy in integers:
        copy.wait()
    def masks(i):
        first = base * rows + (1 - y if i == 0 else y) * block
        qpos = first + lax.broadcasted_iota(jnp.int32, (1, block), 1)
        start = jnp.zeros((1, block), jnp.int32)
        stop = jnp.full((1, block), 1 << 24, jnp.int32)
        end = jnp.int32(0)
        for n in range(length_ref.shape[0]):
            end = end + length_ref[n]
            past = qpos >= end
            start = jnp.where(past, jnp.maximum(start, end), start)
            stop = jnp.where(past, stop, jnp.minimum(stop, end))
        for h in range(heads):
            reach = jnp.full((1, block), HALF * dilation_ref[r * heads + h], jnp.int32)
            lo = jnp.maximum(start - qpos, -reach)
            hi = jnp.minimum(stop - 1 - qpos, reach)
            rel = spaced[h]
            bias[i, h] = jnp.where((rel >= lo) & (rel <= hi), 0.0, NEG)

    with scope("spaced"):
        rel = lax.broadcasted_iota(jnp.int32, (window, block), 0) - halo
        rel = rel - lax.broadcasted_iota(jnp.int32, (window, block), 1)
        relf = rel.astype(F32)
        for h in range(heads):
            spacing = jnp.full((1, block), dilation_ref[r * heads + h], jnp.int32)
            inv = 1.0 / spacing.astype(F32)
            steps = relf * inv
            near = jnp.floor(steps + 0.5)
            spaced[h] = jnp.where(jnp.abs(steps - near) < 0.01, rel, 1 << 24)

    def go_step(mg, weight, first):
        term = lax.dot_general(mg, weight, NT, preferred_element_type=F32)
        if first:
            go_acc[...] = term
        else:
            go_acc[...] += term

    mg_copy.wait()
    w_copy(0).wait()
    for n in range(chunks):
        with scope("go_own"):
            go_step(mg_own[:, part(n)], w_own[:, part(n)], n == 0)

    def go_far(n):
        if n == 0:
            w_copy(1).wait()
        with scope("wait_x"):
            x_copy(n).wait_recv()
        with scope("go_far"):
            go_step(mg_oth[n], w_oth[:, part(n)], False)

    with scope("masks"):
        for i in range(2):
            masks(i)
    with scope("wait_kv"):
        for h in range(heads):
            pass_on(1, h)
        for h in range(heads):
            for o in (2, 3):
                pass_on(o, h)

    def at_rows(i):
        return pl.multiple_of((1 - y) * block if i == 0 else y * block, block)

    def whole(i):
        return pl.ds(at_rows(i), block), pl.ds(0, block)

    def far_part(o):
        return slab(peers[o]), slab(peers[o] - 2 * (1 - y))

    def forward(i, h, q_rows, cols):
        row0 = at_rows(i)
        k = kv[h, 0, pl.ds(row0, window), :]
        v = kv[h, 1, pl.ds(row0, window), :]
        s = lax.dot_general(k, qs[h, q_rows, :], NT, preferred_element_type=F32)
        s = s + bias[i, h, :, cols]
        top = jnp.max(s, axis=0, keepdims=True)
        e = jnp.exp2((s - top) * (factor * LOG2E))
        w = e * (1.0 / jnp.sum(e, axis=0, keepdims=True))
        p = w.astype(BF16)
        probs[i, h, :, cols] = p
        att = lax.dot_general(p, v, TN, preferred_element_type=F32)
        att_my[h, q_rows, :] = att.astype(BF16)

    def att_copy(o, h):
        return remote(
            att_my.at[h, slab(peers[o]), :], att_in.at[:, lanes(r, h)],
            sent, att_recv, peer_id(o),
        )

    def att_local(h):
        return pltpu.make_async_copy(
            att_my.at[h, slab(r), :], att_in.at[:, lanes(r, h)], att_recv
        )

    def near_block(h):
        @pl.when(has_bwd)
        def _():
            with scope("wait_near"):
                arrived(kv.at[h, :, pl.ds(near_row, halo), :], halo_kv.at[0, h])

        for group in ((2,), (3,)) if h == 0 else ((2, 3),):
            with scope("wait_q"):
                for o in group:
                    arrived(qs.at[h, slab(peers[o]), :], q_recv.at[o - 1, h])
            with scope("forward"):
                forward(0, h, *(whole(0) if len(group) == 2 else far_part(group[0])))
            for o in group:
                att_copy(o, h).start()

    def far_blocks():
        @pl.when(has_fwd)
        def _():
            with scope("wait_far"):
                for h in range(heads):
                    arrived(kv.at[h, :, pl.ds(far_row, halo), :], halo_kv.at[1, h])

        with scope("wait_q"):
            for h in range(heads):
                arrived(qs.at[h, pl.ds(at_rows(1), block), :], q_recv.at[0, h])
        with scope("forward"):
            for h in range(heads):
                forward(1, h, *whole(1))
        for h in range(heads):
            att_copy(1, h).start()
            att_local(h).start()

    go_far(0)
    for h in range(heads):
        near_block(h)
    go_far(1)
    far_blocks()
    for n in range(2, chunks - 1):
        go_far(n)

    def go_copy(o, h):
        return remote(
            go_bf.at[:, lanes(peers[o], h)], gos.at[h, slab(r), :],
            sent, go_recv.at[o // 2 * (o - 1), h], peer_id(o),
        )

    def go_local(h):
        return pltpu.make_async_copy(go_bf.at[:, lanes(r, h)], gos.at[h, slab(r), :], go_recv.at[0, h])

    with scope("wait_x"):
        x_copy(chunks - 1).wait_recv()
    for h in range(heads):
        with scope("go_last"):
            for i in range(GROUP):
                at = slice((i * heads + h) * width, (i * heads + h + 1) * width)
                term = lax.dot_general(
                    mg_oth[chunks - 1], w_oth[at, part(chunks - 1)], NT, preferred_element_type=F32
                )
                go_bf[:, at] = (go_acc[:, at] + term).astype(BF16)
        for o in (2, 3, 1):
            go_copy(o, h).start()
        go_local(h).start()

    with scope("wait_att"):
        arrived(att_in, att_recv)

    def p_copy(n, cols):
        return remote(
            part_send.at[n, :, cols], part_recv.at[n, :, cols], sent, p_recv.at[n], x_id
        )

    def project(n, pieces=1):
        size = step // pieces
        for i in range(pieces):
            with scope("proj_far"):
                at = n * step + i * size
                term = jnp.dot(
                    att_in[...], w_oth[:, at : at + size], preferred_element_type=F32
                )
                part_send[n, :, i * size : (i + 1) * size] = term.astype(BF16)
            p_copy(n, pl.ds(i * size, size)).start()

    project(0, 4)

    def edge_rows(i):
        return pl.ds(pl.multiple_of(2 * at_rows(i), block), block)

    def edge_values(i, h):
        go = gos[h, pl.ds(at_rows(i), block), :]
        dv = jnp.dot(probs[i, h, edge_rows(i), :], go, preferred_element_type=F32)
        halo_send[i, h, 1] = dv.astype(BF16)

    def slope_terms(i, h, q_rows, cols):
        v = kv[h, 1, pl.ds(at_rows(i), window), :]
        gp = lax.dot_general(v, gos[h, q_rows, :], NT, preferred_element_type=F32)
        w = probs[i, h, :, cols].astype(F32)
        delta = jnp.sum(w * gp, axis=0, keepdims=True)
        slopes[i, h, :, cols] = (w * (gp - delta)).astype(BF16)

    def edge_keys(i, h):
        q = qs[h, pl.ds(at_rows(i), block), :]
        dk = jnp.dot(slopes[i, h, edge_rows(i), :], q, preferred_element_type=F32) * factor
        halo_send[i, h, 0] = dk.astype(BF16)

    def query_terms(i, h, q_rows, cols):
        k = kv[h, 0, pl.ds(at_rows(i), window), :]
        gq = lax.dot_general(slopes[i, h, :, cols], k, TN, preferred_element_type=F32) * factor
        dq[h, q_rows, :] = gq.astype(BF16)

    def inner_terms(i, h):
        row0 = at_rows(i)
        q = qs[h, pl.ds(row0, block), :]
        go = gos[h, pl.ds(row0, block), :]
        inner = pl.ds(pl.multiple_of(halo - row0, block), 2 * block)
        terms[i, h, 0] = jnp.dot(slopes[i, h, inner, :], q, preferred_element_type=F32) * factor
        terms[i, h, 1] = jnp.dot(probs[i, h, inner, :], go, preferred_element_type=F32)

    def h_copy(i, h, t):
        return remote(
            halo_send.at[i, h, t], halo_recv.at[i, h, t], sent_bwd if i == 0 else sent_fwd,
            h_recv.at[i, h, t], bwd_id if i == 0 else fwd_id,
        )

    results = (gq_ref, gk_ref, gv_ref)

    def out_copy(t, o, h):
        source = dq.at[h] if t == 0 else dkv.at[h, t - 1]
        return remote(
            source.at[slab(peers[o]), :], results[t].at[:, lanes(r, h)],
            sent, out_recv.at[t], peer_id(o),
        )

    def out_local(t, h):
        source = dq.at[h] if t == 0 else dkv.at[h, t - 1]
        return pltpu.make_async_copy(
            source.at[slab(r), :], results[t].at[:, lanes(r, h)], out_recv.at[t]
        )

    def sums(i, t, h):
        @pl.when(has_fwd if i == 0 else has_bwd)
        def _():
            with scope("wait_far_sum" if i else "wait_near_sum"):
                arrived(halo_recv.at[i, h, t], h_recv.at[i, h, t])

        with scope("sums"):
            half = pl.multiple_of(y * block if i == 0 else (1 - y) * block, block)
            out = pl.ds(half, block)
            total = terms[0, h, t, out, :] + terms[1, h, t, out, :]
            total = total + halo_recv[i, h, t].astype(F32)
            dkv[h, t, out, :] = total.astype(BF16)
        if i == 0:
            out_copy(1 + t, 1, h).start()
            out_local(1 + t, h).start()
        else:
            out_copy(1 + t, 2, h).start()
            out_copy(1 + t, 3, h).start()

    def send_edge(t, i, h):
        with scope("edge"):
            (edge_keys, edge_values)[t](i, h)

        @pl.when(has_bwd if i == 0 else has_fwd)
        def _():
            h_copy(i, h, t).start()

    def own_queries(h):
        with scope("wait_go"):
            arrived(gos.at[h, pl.ds(at_rows(1), block), :], go_recv.at[0, h])
        send_edge(1, 1, h)
        with scope("slopes"):
            slope_terms(1, h, *whole(1))
        send_edge(0, 1, h)

    def far_queries(h):
        for group in ((2,), (3,)) if h == 0 else ((2, 3),):
            with scope("wait_go"):
                for o in group:
                    arrived(gos.at[h, slab(peers[o]), :], go_recv.at[o - 1, h])
            with scope("slopes"):
                at = whole(0) if len(group) == 2 else far_part(group[0])
                slope_terms(0, h, *at)
                query_terms(0, h, *at)
            for o in group:
                out_copy(0, o, h).start()

    own_queries(0)
    project(1)
    for h in range(heads):
        far_queries(h)
        send_edge(0, 0, h)
        send_edge(1, 0, h)
        if h > 0:
            sums(1, 0, h - 1)
        with scope("inner"):
            for i in range(2):
                inner_terms(i, h)
        if h + 1 < heads:
            own_queries(h + 1)
        sums(1, 1, h)
        if h + 2 < chunks:
            project(h + 2)
    for n in range(heads + 2, chunks):
        project(n)
    sums(1, 0, heads - 1)
    for h in range(heads):
        with scope("query"):
            query_terms(1, h, *whole(1))
        out_copy(0, 1, h).start()
        out_local(0, h).start()
    with scope("proj_own"):
        for n in range(chunks):
            part_own[n] = jnp.dot(att_in[...], w_own[:, part(n)], preferred_element_type=F32)
    for h in range(heads):
        for t in (1, 0):
            sums(0, t, h)

    def mixed_copy(n):
        return pltpu.make_async_copy(
            mixed_out.at[n], mixed_ref.at[:, part(n)], mixed_sem
        )

    for n in range(chunks):
        with scope("wait_part"):
            arrived(part_recv.at[n], p_recv.at[n])
        with scope("mixed"):
            total = part_own[n] + part_recv[n].astype(F32)
            mixed_out[n] = total.astype(BF16)
        mixed_copy(n).start()

    far_sends = (3 + 1 + 1 + 3) * (GROUP - 1) * rows * heads * width
    sent_rows = (far_sends + 2 * rows * feats) // feats
    arrived(w_own.at[pl.ds(0, sent_rows), :], sent)
    side_rows = (2 * 2 * rows + 2 * halo) * heads * width // feats

    @pl.when(has_fwd)
    def _():
        arrived(w_own.at[pl.ds(0, side_rows), :], sent_fwd)

    @pl.when(has_bwd)
    def _():
        arrived(w_own.at[pl.ds(0, side_rows), :], sent_bwd)

    with scope("end"):
        for t in range(3):
            arrived(results[t], out_recv.at[t])
        arrived(mixed_ref, mixed_sem)


def store_kernel(*refs):
    count = (len(refs) - 1) // 2
    copies = [
        pltpu.make_async_copy(refs[i], refs[count + i], refs[-1].at[i]) for i in range(count)
    ]
    for copy in copies:
        copy.start()
    for copy in copies:
        copy.wait()


def store(arrays):
    place = pl.BlockSpec(memory_space=pltpu.HBM)
    return pl.pallas_call(
        store_kernel,
        in_specs=[pl.BlockSpec(memory_space=pltpu.VMEM)] * len(arrays),
        out_specs=[place] * len(arrays),
        out_shape=[jax.ShapeDtypeStruct(a.shape, a.dtype) for a in arrays],
        scratch_shapes=[pltpu.SemaphoreType.DMA((len(arrays),))],
        compiler_params=pltpu.CompilerParams(vmem_limit_bytes=4 * 1024 * 1024),
    )(*arrays)


def fused(queries, keys, values, out_weight, mixed_grad, lengths, dilation, groups, chunks=4):
    rows, cols = queries.shape
    width = HEAD_WIDTH
    heads = cols // GROUP // width
    feats = mixed_grad.shape[1]
    step = feats // chunks
    block, halo, tokens = 2 * rows, 2 * rows, GROUP * rows
    window = block + 2 * halo
    hbm = pl.BlockSpec(memory_space=pltpu.HBM)
    vmem = pl.BlockSpec(memory_space=pl.ANY)
    dma = pltpu.SemaphoreType.DMA
    V = pltpu.VMEM
    one = jax.ShapeDtypeStruct((rows, cols), BF16)
    big = [
        pltpu.with_memory_space_constraint(a, pltpu.HBM)
        for a in (lengths, dilation, queries, keys, values, out_weight, mixed_grad)
    ]
    outs = pl.pallas_call(
        functools.partial(fused_kernel, groups),
        in_specs=[hbm] * 7,
        out_specs=[vmem] * 4,
        out_shape=[jax.ShapeDtypeStruct((rows, feats), BF16), one, one, one],
        scratch_shapes=[
            V((cols, feats), BF16), V((cols, feats), BF16),
            V((rows, feats), BF16), V((chunks, rows, step), BF16),
            V((heads, 2, tokens + 2 * halo, width), BF16),
            V((heads, tokens, width), BF16), V((heads, tokens, width), BF16),
            V((rows, cols), F32), V((rows, cols), BF16),
            V((heads, tokens, width), BF16), V((rows, cols), BF16),
            V((chunks, rows, step), BF16), V((chunks, rows, step), BF16), V((chunks, rows, step), F32),
            V((2, heads, window, block), BF16), V((heads, window, block), jnp.int32),
            V((2, heads, window, block), F32), V((2, heads, 2, 2 * block, width), F32),
            V((2, heads, window, block), BF16),
            V((2, heads, 2, halo, width), BF16), V((2, heads, 2, halo, width), BF16),
            V((heads, tokens, width), BF16), V((heads, 2, tokens, width), BF16),
            V((chunks, rows, step), BF16), pltpu.SMEM(lengths.shape, jnp.int32), pltpu.SMEM(dilation.shape, jnp.int32),
            dma((2,)), dma((2,)), dma, dma, dma((chunks,)), dma((GROUP - 1, heads)), dma((3, heads)),
            dma((2, heads)), dma((3, heads)), dma, dma((chunks,)), dma((2, heads, 2)), dma((3,)), dma,
            dma, dma, dma,
        ],
        compiler_params=pltpu.CompilerParams(
            collective_id=0, has_side_effects=True, vmem_limit_bytes=32 * 1024 * 1024
        ),
    )(*big)
    return tuple(store(outs))


def attend_kernel(
    row_count, total, factor, first, index_ref, length_ref, dilation_ref,
    q_ref, go_ref, own_ref, a_ref, b_ref, po_ref, pa_ref,
    att_ref, gq_ref, own_t, a_t, b_t, po_t, pa_t, dist,
):
    slabs = (own_ref, a_ref, b_ref, po_ref, pa_ref)
    outs = (own_t, a_t, b_t, po_t, pa_t)

    @pl.when(pl.program_id(0) == 0)
    def _():
        me = index_ref[0]
        sign = 1 - 2 * lax.rem(me, 2)
        ends = [length_ref[0]]
        for n in range(1, length_ref.shape[0]):
            ends.append(ends[-1] + length_ref[n])

        def segment(pos):
            seg = jnp.zeros(pos.shape, jnp.int32)
            for end in ends:
                seg = seg + (pos >= end).astype(jnp.int32)
            return seg

        qpos = me * row_count + lax.broadcasted_iota(jnp.int32, (1, row_count), 1)
        qseg = segment(qpos)
        for i, off in enumerate((0, 2, -2, 1, -1)):
            kpos = (me + sign * off) * row_count + lax.broadcasted_iota(
                jnp.int32, (row_count, row_count), 0
            )
            same = (segment(kpos) == qseg) & (kpos >= 0) & (kpos < total)
            gap = jnp.abs(kpos - qpos).astype(jnp.float32)
            dist[pl.ds(i * row_count, row_count), :] = jnp.where(same, gap, FAR)

    spacing = jnp.full((1, row_count), dilation_ref[first + pl.program_id(0)], jnp.int32)
    inv = 1.0 / spacing.astype(jnp.float32)
    steps = dist[...] * inv
    whole = jnp.floor(steps + 0.5)
    mask = (whole <= HALF) & (jnp.abs(steps - whole) < 0.01)
    q = q_ref[...]
    go = go_ref[...]
    k = jnp.concatenate([r[0] for r in slabs], axis=0)
    v = jnp.concatenate([r[1] for r in slabs], axis=0)
    nt = (((1,), (1,)), ((), ()))
    tn = (((0,), (0,)), ((), ()))
    f32 = jnp.float32
    scores = lax.dot_general(k, q, nt, preferred_element_type=f32) * factor
    scores = jnp.where(mask, scores, NEG)
    top = jnp.max(scores, axis=0, keepdims=True)
    e = jnp.exp(scores - top)
    w = e * (1.0 / jnp.sum(e, axis=0, keepdims=True))
    p = w.astype(jnp.bfloat16)
    gp = lax.dot_general(v, go, nt, preferred_element_type=f32)
    delta = jnp.sum(w * gp, axis=0, keepdims=True)
    s = (w * (gp - delta)).astype(jnp.bfloat16)
    att_ref[...] = lax.dot_general(p, v, tn, preferred_element_type=f32).astype(jnp.bfloat16)
    gq_ref[...] = (
        lax.dot_general(s, k, tn, preferred_element_type=f32) * factor
    ).astype(jnp.bfloat16)
    kt = (jnp.dot(s, q, preferred_element_type=f32) * factor).astype(jnp.bfloat16)
    vt = jnp.dot(p, go, preferred_element_type=f32).astype(jnp.bfloat16)
    for i, out in enumerate(outs):
        out[0] = kt[i * row_count : (i + 1) * row_count]
        out[1] = vt[i * row_count : (i + 1) * row_count]


def attend(index, lengths, dilation, q, go, slabs, first, total, factor, width):
    rows, cols = q.shape[0], slabs[0].shape[2]
    heads = cols // width
    smem = pl.BlockSpec(memory_space=pltpu.SMEM)
    shared = pl.BlockSpec((rows, width), lambda h: (0, first + h))
    flat = pl.BlockSpec((rows, width), lambda h: (0, h))
    pair = pl.BlockSpec((2, rows, width), lambda h: (0, 0, h))
    one = jax.ShapeDtypeStruct((rows, cols), jnp.bfloat16)
    two = jax.ShapeDtypeStruct((2, rows, cols), jnp.bfloat16)
    return pl.pallas_call(
        functools.partial(attend_kernel, rows, total, factor, first),
        grid=(heads,),
        in_specs=[smem, smem, smem, shared, shared] + [pair] * 5,
        out_specs=[flat, flat] + [pair] * 5,
        out_shape=[one, one] + [two] * 5,
        scratch_shapes=[pltpu.VMEM((5 * rows, rows), jnp.float32)],
        compiler_params=pltpu.CompilerParams(dimension_semantics=("arbitrary",)),
        cost_estimate=pl.CostEstimate(
            flops=heads * 6 * 2 * 5 * rows * rows * width * 8,
            bytes_accessed=24 * 2 * rows * cols,
            transcendentals=heads * 5 * rows * rows,
        ),
    )(index, lengths, dilation, q, go, *slabs)


def per_device(queries, keys, values, out_weight, mixed_grad, lengths, dilation):
    rows = queries.shape[0]
    local_heads = dilation.shape[0]
    width = queries.shape[1] // local_heads
    factor = width ** (-0.5)
    count = lax.axis_size("ctx")
    sides = lax.axis_size("head")
    total = rows * count
    assert 2 * rows >= HALF * MAXD and count % 2 == 0
    if sides == 2 and count % GROUP == 0 and local_heads % GROUP == 0 and width == HEAD_WIDTH:
        if 2 * rows == HALF * MAXD and mixed_grad.shape[1] % 512 == 0:
            return fused(
                queries, keys, values, out_weight, mixed_grad, lengths, dilation, count // GROUP
            )
    index = lax.axis_index("ctx").astype(jnp.int32).reshape(1)

    inward = [
        (j, t) for j in range(count) for t in [j - 2 if j % 2 == 0 else j + 2] if 0 <= t < count
    ]
    outward = [(t, j) for j, t in inward]
    swapped = [(j, j ^ 1) for j in range(count)]

    def move(x, pairs):
        return lax.ppermute(x, "ctx", pairs)

    groups = 1
    gh = local_heads // groups
    cut = [slice(g * gh * width, (g + 1) * gh * width) for g in range(groups)]
    half = mixed_grad.shape[1]
    if sides == 2:
        other = lax.ppermute(mixed_grad, "head", [(0, 1), (1, 0)])
        left = lax.axis_index("head") == 0
        grad_full = jnp.concatenate(
            [jnp.where(left, mixed_grad, other), jnp.where(left, other, mixed_grad)], axis=1
        )
    else:
        grad_full = lax.all_gather(mixed_grad, "head", axis=1, tiled=True)
    stacks = []
    for g in range(groups):
        own = jnp.stack([keys[:, cut[g]], values[:, cut[g]]])
        stacks.append([own, move(own, inward), move(own, outward), move(own, swapped)])
    grad_attention = lax.dot_general(
        grad_full, out_weight, (((1,), (1,)), ((), ())), preferred_element_type=jnp.float32
    ).astype(jnp.bfloat16)

    atts, gqs, gkvs = [], [], []
    f32 = jnp.float32
    for slabs in stacks:
        slabs[1], grad_attention = lax.optimization_barrier((slabs[1], grad_attention))
        slabs.append(move(slabs[1], swapped))
    for g in range(groups):
        att, gq, own_t, a_t, b_t, po_t, pa_t = attend(
            index, lengths, dilation, queries, grad_attention, stacks[g], g * gh, total, factor, width
        )
        pa_back = move(pa_t, swapped)
        b_back = move(b_t, inward)
        po_back = move(po_t, swapped)
        a_sum = (a_t.astype(f32) + pa_back.astype(f32)).astype(jnp.bfloat16)
        a_sum, att = lax.optimization_barrier((a_sum, att))
        a_back = move(a_sum, outward)
        terms = (own_t, po_back, b_back, a_back)
        gkvs.append(
            [sum(term[i].astype(f32) for term in terms).astype(jnp.bfloat16) for i in range(2)]
        )
        atts.append(att)
        gqs.append(gq)
    attention = jnp.concatenate(atts, axis=1)
    partial = jnp.dot(attention, out_weight, preferred_element_type=f32)
    if sides == 2:
        lo, hi = partial[:, :half], partial[:, half:]
        away = jnp.where(left, hi, lo).astype(jnp.bfloat16)
        came = lax.ppermute(away, "head", [(0, 1), (1, 0)])
        mixed = (jnp.where(left, lo, hi) + came.astype(f32)).astype(jnp.bfloat16)
    else:
        mixed = lax.psum_scatter(
            partial.astype(jnp.bfloat16), "head", scatter_dimension=1, tiled=True
        )
    grad_keys, grad_values = (
        jnp.concatenate([pair[i] for pair in gkvs], axis=1) for i in range(2)
    )
    return mixed, jnp.concatenate(gqs, axis=1), grad_keys, grad_values


def solution(mesh):
    both = P("ctx", "head")
    return jax.shard_map(
        per_device,
        mesh=mesh,
        in_specs=(both, both, both, P("head", None), both, P(), P("head")),
        out_specs=(both, both, both, both),
        check_vma=False,
    )
```
